32 devices in a mesh: seq: 8 (over z, x), head: 4 (over y, core).
Axes of the slice: x: 2, y: 2, z: 4, core: 2. Of those that a mesh axis runs over, the one named last changes fastest.
Arguments:
- queries: bfloat16 [8192, 4096], P('seq', 'head'), may hold values from -150 to 150
- keys: bfloat16 [8192, 4096], P('seq', 'head'), may hold values from -7 to 7
- values: bfloat16 [8192, 4096], P('seq', 'head'), may hold values from -6 to 6
- random_holder: int32 [32, 64, 3], P('head', 'seq'), may hold values from 0 to 7, all different within a row; in each aligned block of 8 rows (0 to 7, 8 to 15, ..., all dimensions but the last counted through in order) at most 3 rows name the same one
- random_offset: int32 [32, 64, 3], P('head', 'seq'), may hold values from 0 to 7
- keep: int32 [64], P('seq'), may hold values from 0 to 1, as said below
Outputs:
- packed: bfloat16 [8192, 4096], P('seq', 'head')
The draws below stay inside these ranges and needn't reach their ends.
Inputs may be any that keep to these rules, and one draw needn't show every extreme that they name: `random_holder`: for each head, the 8 query blocks of one index of seq name no index of seq more than 3 times over all their random entries; the 3 entries of one query block and head differ. `keep`: block j is kept where j % 8 == 0 or j % 8 == 7, and not kept where j % 8 == 1.
All inputs are finite; a program needn't handle non-finite values.
Results may differ from the reference program's by a relative error of at most 0.007.
Values may be sent and summed in bfloat16 or wider, within the bound.
No kernel may reach another device: no remote copies, remote signals or barrier semaphores. Data moves between devices by JAX's collectives and lax.ppermute only.
A program may use at most 128 MiB of HBM per device.

```python
import math
import jax
import jax.numpy as jnp
import numpy as np
from jax import lax

H = 32
DH = 128
B = 128
G = 2
R = 3
BD = 8
NB = 64
L = 8192
MOST = 3
N_SEQ = 8


def paired_rows(key):
    base = jax.random.fold_in(key, 71)
    key_rows = jnp.clip(jax.random.normal(jax.random.fold_in(base, 1), (L, H * DH), jnp.float32), -6.0, 6.0)
    query_rows = jnp.clip(jax.random.normal(jax.random.fold_in(base, 2), (L, H * DH), jnp.float32), -6.0, 6.0)
    return (query_rows, key_rows)


def draw_queries(key, part):
    query_rows, key_rows = paired_rows(key)
    return query_rows.astype(jnp.bfloat16)


def draw_keys(key, part):
    query_rows, key_rows = paired_rows(key)
    return key_rows.astype(jnp.bfloat16)


def draw_keep(key, part):
    count = L // B
    rolled = jax.random.randint(jax.random.fold_in(key, 113), (count,), 0, 3)
    kept = (rolled == 0).astype(jnp.int32)
    position = jnp.arange(count, dtype=jnp.int32) % BD
    kept = jnp.where(position == 0, 1, kept)
    kept = jnp.where(position == BD - 1, 1, kept)
    kept = jnp.where(position == 1, 0, kept)
    return kept.astype(jnp.int32)


def plant(array, key, smallest, largest):
    extent = array.shape
    spot = [jax.random.randint(jax.random.fold_in(key, axis), (), 0, extent[axis]) for axis in range(len(extent))]
    array = array.at[tuple(spot)].set(smallest)
    longest = extent.index(max(extent))
    spot[longest] = (spot[longest] + 1) % extent[longest]
    return array.at[tuple(spot)].set(largest)


def levels(rng, shape, split, low, high):
    gain = 1.0
    for dim, shards_of in split:
        heights = jax.random.uniform(jax.random.fold_in(jax.random.fold_in(rng, 6), dim), (shards_of,), jnp.float32, low / len(split), high / len(split))
        gain = gain * jnp.repeat(jnp.exp(heights), shape[dim] // shards_of).reshape((-1,) + (1,) * (len(shape) - 1 - dim))
    return gain


def shared_out(rng, own, number, rows, number_of, top, limit, slope):
    sequence = jax.random.permutation(rng, number_of)
    heavy_load, usual = shares(number_of, rows * top, limit, slope, True), shares(number_of, rows * top, limit, slope, False)
    places = jnp.arange(number_of)

    def named(sizes, offset_by):
        used = int((sizes > 0).sum())
        fixed = max(1, used // 4)
        shifted = fixed + (places - fixed + offset_by * (used - fixed)) % max(1, number_of - fixed)
        return jnp.zeros((number_of,), jnp.int32).at[sequence[jnp.where(places < fixed, places, shifted)]].set(jnp.asarray(sizes, jnp.int32))

    sizes = jnp.where(number % 4 == 0, named(heavy_load, number // 4), named(usual, number - number // 4 - 1))
    mixed = jax.random.permutation(jax.random.fold_in(own, 3), number_of)
    source_of, sink = mixed[0:number_of // 2 * 2:2], mixed[1:number_of // 2 * 2:2]
    slack = jnp.minimum(sizes[source_of] - 1, limit - sizes[sink]) // 2
    slack = jnp.where((source_of == sequence[0]) | (sink == sequence[0]) | (sizes[sink] == 0), 0, jnp.maximum(slack, 0))
    shifted = jax.random.randint(jax.random.fold_in(own, 4), (number_of // 2,), 0, 1 << 20) % (slack + 1)
    sizes = sizes.at[source_of].add(-shifted).at[sink].add(shifted)
    labels = jnp.searchsorted(jnp.cumsum(sizes), jnp.arange(rows * top), side="right").astype(jnp.int32)
    table = labels.reshape(top, rows).T
    table = table[jax.random.permutation(jax.random.fold_in(own, 1), rows)]
    offset_by = jax.random.randint(jax.random.fold_in(own, 2), (rows, 1), 0, top)
    return jnp.take_along_axis(table, (jnp.arange(top)[None, :] + offset_by) % top, axis=1)


def shares(amount, total, limit, skew, full):
    weights = [(1 << 20) // math.isqrt(standing ** skew) + 1 for standing in range(1, amount + 1)]
    largest = limit if full else min(limit, max(-(-total // amount), total * weights[0] // sum(weights)))
    least = 1 if total - largest >= amount - 1 else 0
    counts, spare = [largest] + [least] * (amount - 1), total - largest - least * (amount - 1)
    while spare > 0:
        movable = [i for i in range(1, amount) if counts[i] < largest] or [i for i in range(1, amount) if counts[i] < limit]
        whole, left = sum([weights[i] for i in movable]), spare
        for i in movable:
            more = min(limit - counts[i], max(1, left * weights[i] // whole), spare)
            counts[i] = counts[i] + more
            spare = spare - more
    return np.array(counts)


def bell_draw(rng, dims, deviation, bound, split=(), kind=jnp.bfloat16):
    drawn = jax.random.normal(rng, dims, jnp.float32) * deviation
    if len(split) > 0:
        drawn = levels(rng, dims, split, -0.22, 0.18) * drawn
    return jnp.clip(drawn, min=-bound, max=bound).astype(kind)


def setup_inputs(seed: int = 0) -> dict:
    key_of = jax.random.split(jax.random.key(seed), 7)
    queries = draw_queries(jax.random.fold_in(key_of[6], 71), 0)
    keys = draw_keys(jax.random.fold_in(key_of[6], 71), 0)
    values = bell_draw(key_of[2], (L, H * DH), 1.0, 6.0, ((0, 8), (1, 4)))
    random_holder_keys = jax.random.split(jax.random.fold_in(key_of[3], 1), H * NB // BD)
    random_holder_turns = jax.random.permutation(jax.random.fold_in(key_of[3], 3), H * NB // BD)
    random_holder = jax.vmap(lambda own, number: shared_out(jax.random.fold_in(key_of[3], 2), own, number, BD, N_SEQ, R, MOST, 2))(random_holder_keys, random_holder_turns).reshape((H, NB, R))
    random_offset = plant(jax.random.randint(key_of[4], (H, NB, R), 0, BD), jax.random.fold_in(key_of[4], 1), 0, BD - 1).astype(jnp.int32)
    keep = draw_keep(jax.random.fold_in(key_of[6], 71), 0)
    return {"queries": queries, "keys": keys, "values": values, "random_holder": random_holder, "random_offset": random_offset, "keep": keep}


neg_big = -1.0e30


def reference(queries, keys, values, random_holder, random_offset, keep):
    score_scale = 1.0 / (DH ** 0.5)
    query_blocks = queries.reshape(NB, B, H, DH)
    key_blocks = keys.reshape(NB, B, H, DH)
    value_blocks = values.reshape(NB, B, H, DH)
    head_idx = jnp.arange(H, dtype=jnp.int32)[:, None]

    def one_block(block_idx):
        left = jnp.maximum(block_idx - 1, 0)
        right = jnp.minimum(block_idx + 1, NB - 1)
        common = jnp.concatenate((jnp.stack((left, block_idx, right)).astype(jnp.int32), jnp.arange(G, dtype=jnp.int32)))
        common_keys = jnp.transpose(key_blocks[common], (0, 2, 1, 3))
        common_values = jnp.transpose(value_blocks[common], (0, 2, 1, 3))
        chosen = (random_holder[:, block_idx] * BD + random_offset[:, block_idx]).astype(jnp.int32)
        rand_keys = jnp.transpose(key_blocks[chosen, :, head_idx, :], (1, 0, 2, 3))
        rand_values = jnp.transpose(value_blocks[chosen, :, head_idx, :], (1, 0, 2, 3))
        tile_keys = jnp.concatenate((common_keys, rand_keys), axis=0).astype(jnp.float32)
        tile_values = jnp.concatenate((common_values, rand_values), axis=0).astype(jnp.float32)
        live = jnp.concatenate((jnp.stack((block_idx > 0, block_idx >= 0, block_idx < NB - 1)), jnp.ones((G + R,), dtype=bool)))
        query_tile = jnp.transpose(query_blocks[block_idx], (1, 0, 2)).astype(jnp.float32)
        scores = jnp.einsum('hqd,thkd->thqk', query_tile, tile_keys) * score_scale
        row_max = jnp.max(scores, axis=-1)
        weights = jnp.exp(scores - row_max[..., None]).astype(jnp.bfloat16).astype(jnp.float32)
        row_sum = jnp.sum(weights, axis=-1)
        summed = jnp.einsum('thqk,thkd->thqd', weights, tile_values)
        live_b = live[:, None, None]
        overall = jnp.max(jnp.where(live_b, row_max, neg_big), axis=0)
        factor = jnp.where(live_b, jnp.exp(row_max - overall[None]), 0.0)
        numer = jnp.sum(factor[..., None] * summed, axis=0)
        denom = jnp.sum(factor * row_sum, axis=0)
        result = numer / denom[..., None]
        return jnp.transpose(result, (1, 0, 2)).reshape(B, H * DH).astype(jnp.bfloat16)

    attended = lax.map(one_block, jnp.arange(NB, dtype=jnp.int32))
    keep_i = keep.astype(jnp.int32)
    local_rank = (jnp.cumsum(keep_i) - keep_i).astype(jnp.int32)
    place = jnp.where(keep_i > 0, local_rank, NB).astype(jnp.int32)
    packed = jnp.zeros((NB + 1, B, H * DH), jnp.bfloat16).at[place].set(attended)
    return packed[:NB].reshape(L, H * DH)
```

```python
import functools
import math

import jax
import jax.numpy as jnp
from jax import lax
from jax.experimental import pallas as pl
from jax.experimental.pallas import tpu as pltpu
from jax.sharding import PartitionSpec as P

DH = 128
B = 128
G = 2
R = 3
LANES = 128

neg_big = -1e30

ROUTE_SHARES = ((0.66, 0.545, 0.61), (0.73, 0.6, 0.7), (1.0, 1.0, 1.0))
PACK_SHARES = ((0.72, 0.36, 0.75), (1.0, 1.0, 1.0))


def log2(size):
    assert size & (size - 1) == 0
    return size.bit_length() - 1


class Plan:
    def __init__(self, count, groups, blk_dev, head_dev):
        self.count, self.groups, self.blk, self.heads = count, groups, blk_dev, head_dev
        self.bits = log2(count)
        self.stride = groups * head_dev
        self.lanes = count * self.stride
        self.blocks = count * blk_dev
        self.req = blk_dev * R
        self.per_head = blk_dev + 2 + G
        self.own = blk_dev * head_dev
        most = max(2, (self.req + count - 1) // count)
        bound = (count // 2) * most * head_dev
        self.full = [min(self.own << s, bound) for s in range(self.bits)]
        self.base = [sum(self.full[:s]) for s in range(self.bits)]
        self.pool = head_dev * self.per_head + sum(self.full)
        self.cfull = [
            min((blk_dev - 1) << s, blk_dev << (self.bits - 1 - s)) for s in range(self.bits)
        ]
        self.cbase = [sum(self.cfull[:s]) for s in range(self.bits)]
        self.width = -(-max(self.full + self.cfull) // LANES) * LANES

    def sizes(self, full, shares):
        out = []
        for s in range(self.bits):
            share = shares[0] if s == 0 else shares[2] if s == self.bits - 1 else shares[1]
            out.append(min(full[s], max(1, math.ceil(full[s] * share))))
        return out

    def route_sizes(self):
        return [self.sizes(self.full, shares) for shares in ROUTE_SHARES]

    def pack_sizes(self):
        return [self.sizes(self.cfull, shares) for shares in PACK_SHARES]

    def rows(self):
        return 2 * self.bits + 4


def iota(shape, axis):
    return lax.broadcasted_iota(jnp.int32, shape, axis)


def flag(cond):
    return jnp.where(cond, 1.0, 0.0)


def dot(a, b):
    return jnp.dot(
        a.astype(jnp.bfloat16), b.astype(jnp.bfloat16), preferred_element_type=jnp.float32
    )


def choose(tops, sizes):
    index = jnp.int32(len(sizes) - 1)
    for number in reversed(range(len(sizes) - 1)):
        fits = functools.reduce(
            jnp.logical_and, [top <= float(size) for top, size in zip(tops, sizes[number])]
        )
        index = jnp.where(fits, jnp.int32(number), index)
    return index


def lists_body(plan, scal, ids, own_ids, lists, table):
    me, group = scal[0], scal[1]
    T, L, hd = plan.blocks, plan.lanes, plan.heads
    lb, ls, lh = log2(plan.blk), log2(plan.stride), log2(hd)
    W = plan.width
    t = iota((T, L), 0)
    lane = iota((T, L), 1)
    holder = jnp.right_shift(lane, ls)
    need = jnp.zeros((T, L), jnp.int32)
    for k in range(plan.req):
        need = jnp.where(t == ids[k : k + 1, :], 1, need)
    near = (t >= holder * plan.blk - 1) & (t <= (holder + 1) * plan.blk)
    need = jnp.where(near | (t < G), 0, need)
    needb = need.astype(jnp.float32).astype(jnp.bfloat16)
    x = iota((L, L), 0)
    y = iota((L, L), 1)
    lower = flag(iota((T, T), 0) > iota((T, T), 1)).astype(jnp.bfloat16)
    upper = flag(iota((hd, hd), 0) < iota((hd, hd), 1)).astype(jnp.bfloat16)
    same = flag(jnp.right_shift(x, lh) == jnp.right_shift(y, lh)).astype(jnp.bfloat16)
    xe = iota((L, hd), 0)
    he = iota((L, hd), 1)
    th = iota((T, hd), 0)
    hh = iota((T, hd), 1)
    blk_of = jnp.right_shift(th, lb)
    pos_of = th & (plan.blk - 1)
    is_own = blk_of == me
    loc = jnp.where(is_own, jnp.left_shift(hh, lb) + pos_of, 0)
    slot_w = iota((T, W), 1)
    tops = []

    def order(mask):
        within = jnp.dot(lower, mask.astype(jnp.bfloat16), preferred_element_type=jnp.float32)
        cols = jnp.broadcast_to(jnp.sum(mask, axis=0, keepdims=True), (8, hd))
        return within + dot(cols, upper)[0:1, :]

    for s in range(plan.bits):
        b = plan.bits - 1 - s
        free = ((1 << b) - 1) << ls
        group_of = flag(((x ^ y) & ~free) == 0).astype(jnp.bfloat16)
        wanted = jnp.dot(needb, group_of, preferred_element_type=jnp.float32)
        into = ((jnp.right_shift(t, lb) ^ holder ^ (1 << b)) & ((2 << b) - 1)) == 0
        recv = flag((wanted > 0.5) & into)
        cols = jnp.broadcast_to(jnp.sum(recv, axis=0, keepdims=True), (8, L))
        tops.append(jnp.max(dot(cols, same)))
        recvb = recv.astype(jnp.bfloat16)
        mine = flag(xe == me * plan.stride + group * hd + he).astype(jnp.bfloat16)
        theirs = flag(xe == (me ^ (1 << b)) * plan.stride + group * hd + he).astype(jnp.bfloat16)
        got = jnp.dot(recvb, mine, preferred_element_type=jnp.float32)
        sent = jnp.dot(recvb, theirs, preferred_element_type=jnp.float32)
        place = jnp.where(sent > 0.5, order(sent).astype(jnp.int32), -1)
        line = jnp.zeros((1, W), jnp.int32)
        for h in range(hd):
            hit = place[:, h : h + 1] == slot_w
            line = line + jnp.sum(
                jnp.where(hit, loc[:, h : h + 1] + 1, 0), axis=0, keepdims=True
            )
        lists[s : s + 1, :] = line
        loc = jnp.where(
            got > 0.5, plan.own + plan.base[s] + order(got).astype(jnp.int32), loc
        )
    per = plan.per_head
    at = jnp.where(is_own, hh * per + 1 + pos_of, loc + hd * (per - plan.blk))
    at = jnp.where(th == me * plan.blk - 1, hh * per, at)
    at = jnp.where(th == (me + 1) * plan.blk, hh * per + 1 + plan.blk, at)
    at = jnp.where((th < G) & ~is_own, hh * per + 2 + plan.blk + th, at)
    for k in range(plan.req):
        hit = th == own_ids[k : k + 1, :]
        table[k : k + 1, 0:hd] = jnp.sum(jnp.where(hit, at, 0), axis=0, keepdims=True)

    kept = jnp.zeros((T, L), jnp.int32)
    head_lane = (jnp.right_shift(t, lb) == holder) & ((lane & (plan.stride - 1)) == 0)
    for i in range(plan.blk):
        hit = head_lane & ((t & (plan.blk - 1)) == i)
        kept = kept + jnp.where(hit, ids[plan.req + i : plan.req + i + 1, :], 0)
    kept = jnp.broadcast_to(jnp.sum(kept, axis=1, keepdims=True), (T, W))
    tw = iota((T, W), 0)
    dev = jnp.right_shift(tw, lb)

    def before(mask):
        return jnp.dot(
            lower, mask.astype(jnp.float32).astype(jnp.bfloat16), preferred_element_type=jnp.float32
        ).astype(jnp.int32)

    rank = before(kept)
    dest = jnp.right_shift(rank, lb)
    cloc = jnp.where(dev == me, tw & (plan.blk - 1), 0)
    ctops = []
    for s in range(plan.bits):
        b = plan.bits - 1 - s
        ok = (kept > 0) & (jnp.right_shift(dest ^ slot_w, b) == 0)
        ok = ok & (((dev ^ slot_w ^ (1 << b)) & ((2 << b) - 1)) == 0)
        recv = jnp.where(ok, 1, 0)
        ctops.append(jnp.max(jnp.sum(recv.astype(jnp.float32), axis=0, keepdims=True)))
        got = jnp.sum(jnp.where(slot_w == me, recv, 0), axis=1, keepdims=True)
        sent = jnp.sum(jnp.where(slot_w == (me ^ (1 << b)), recv, 0), axis=1, keepdims=True)
        got = jnp.broadcast_to(got, (T, W))
        sent = jnp.broadcast_to(sent, (T, W))
        hit = (sent > 0) & (before(sent) == slot_w)
        row = plan.bits + s
        lists[row : row + 1, :] = jnp.sum(jnp.where(hit, cloc + 1, 0), axis=0, keepdims=True)
        cloc = jnp.where(got > 0, plan.blk + plan.cbase[s] + before(got), cloc)
    row = 2 * plan.bits
    hit = (kept > 0) & (rank == me * plan.blk + slot_w) & (slot_w < plan.blk)
    lists[row : row + 1, :] = jnp.sum(jnp.where(hit, cloc + 1, 0), axis=0, keepdims=True)
    chosen = jnp.where(
        iota((1, W), 1) == 0,
        choose(tops, plan.route_sizes()),
        choose(ctops, plan.pack_sizes()),
    )
    lists[row + 1 : row + 2, :] = chosen
    first = jnp.sum(jnp.where(tw < me * plan.blk, kept, 0), axis=0, keepdims=True)
    hit = (kept > 0) & (dev == me) & (rank - first == slot_w)
    lists[row + 2 : row + 3, :] = jnp.sum(
        jnp.where(hit, tw & (plan.blk - 1), 0), axis=0, keepdims=True
    )
    lists[row + 3 : row + 4, :] = jnp.sum(
        jnp.where((dev == me), kept, 0), axis=0, keepdims=True
    )


SMEM = pl.BlockSpec(memory_space=pltpu.SMEM)
VMEM = pl.BlockSpec(memory_space=pltpu.VMEM)
ANY = pl.BlockSpec(memory_space=pl.ANY)


def make_lists(plan, scal, ids, own_ids):
    return pl.pallas_call(
        functools.partial(lists_body, plan),
        out_shape=(
            jax.ShapeDtypeStruct((plan.rows(), plan.width), jnp.int32),
            jax.ShapeDtypeStruct((plan.req, LANES), jnp.int32),
        ),
        in_specs=[SMEM, VMEM, VMEM],
        out_specs=(VMEM, VMEM),
        name="make_lists",
    )(scal, ids, own_ids)


def copy_tile(code, sources, bases, own_shape, target, sem, heads_bits):
    own = sources[0]

    @pl.when(code < bases[0])
    def _():
        if heads_bits is None:
            part = own.at[pl.ds(pl.multiple_of(code * B, B), B), :]
        else:
            head = jnp.right_shift(code, heads_bits)
            pos = code & ((1 << heads_bits) - 1)
            part = own.at[
                pl.ds(pl.multiple_of(pos * B, B), B), pl.ds(pl.multiple_of(head * DH, DH), DH)
            ]
        pltpu.make_async_copy(part, target, sem).start()

    for number, source in enumerate(sources[1:]):
        low = bases[number]
        high = bases[number + 1]

        @pl.when((code >= low) & (code < high))
        def _():
            at = pl.multiple_of((code - low) * B, B)
            pltpu.make_async_copy(source.at[pl.ds(at, B), :], target, sem).start()


def pack_body(row, size, bases, heads_bits, lists, *refs):
    sources, out, sem = refs[:-2], refs[-2], refs[-1]

    def step(j, carry):
        code = jnp.maximum(lists[row, j] - 1, 0)
        target = out.at[pl.ds(pl.multiple_of(j * B, B), B), :]
        copy_tile(code, sources, bases, None, target, sem, heads_bits)
        return carry

    lax.fori_loop(0, size, step, 0)
    pltpu.make_async_copy(out, out, sem).wait()


def pack(row, size, bases, heads_bits, lists, sources, width, name):
    return pl.pallas_call(
        functools.partial(pack_body, row, size, bases, heads_bits),
        out_shape=jax.ShapeDtypeStruct((size * B, width), jnp.bfloat16),
        in_specs=[SMEM] + [ANY] * len(sources),
        out_specs=ANY,
        scratch_shapes=[pltpu.SemaphoreType.DMA],
        name=name,
    )(lists, *sources)


def final_body(row, slots, bases, lists, *refs):
    sources, out, zeros, sem = refs[:-3], refs[-3], refs[-2], refs[-1]
    zeros[...] = jnp.zeros_like(zeros)

    def step(j, carry):
        code = lists[row, j]
        target = out.at[pl.ds(pl.multiple_of(j * B, B), B), :]

        @pl.when(code == 0)
        def _():
            pltpu.make_async_copy(zeros, target, sem).start()

        @pl.when(code > 0)
        def _():
            copy_tile(code - 1, sources, bases, None, target, sem, None)

        return carry

    lax.fori_loop(0, slots, step, 0)
    pltpu.make_async_copy(out, out, sem).wait()


def final(row, slots, bases, lists, sources, width):
    return pl.pallas_call(
        functools.partial(final_body, row, slots, bases),
        out_shape=jax.ShapeDtypeStruct((slots * B, width), jnp.bfloat16),
        in_specs=[SMEM] + [ANY] * len(sources),
        out_specs=ANY,
        scratch_shapes=[pltpu.VMEM((B, width), jnp.bfloat16), pltpu.SemaphoreType.DMA],
        name="place_blocks",
    )(lists, *sources)


def attend_body(plan, sizes, lists, table, scal, q, *refs):
    count = 8 + 2 * plan.bits
    ins, out, pools, sem = refs[:count], refs[count], refs[count + 1 : count + 3], refs[count + 3]
    blk, hd, per = plan.blk, plan.heads, plan.per_head
    copies = []
    for which in range(2):
        own, low, high, shared = ins[4 * which : 4 * which + 4]
        pool = pools[which]
        for h in range(hd):
            cols = pl.ds(h * DH, DH)
            for source, at, tiles in (
                (low, 0, 1),
                (own, 1, blk),
                (high, 1 + blk, 1),
                (shared, 2 + blk, G),
            ):
                copies.append(
                    pltpu.make_async_copy(
                        source.at[:, cols],
                        pool.at[pl.ds((h * per + at) * B, tiles * B), :],
                        sem.at[len(copies)],
                    )
                )
        for s in range(plan.bits):
            at = (hd * per + plan.base[s]) * B
            copies.append(
                pltpu.make_async_copy(
                    ins[8 + which * plan.bits + s],
                    pool.at[pl.ds(at, sizes[s] * B), :],
                    sem.at[len(copies)],
                )
            )
    for copy in copies:
        copy.start()
    for copy in copies:
        copy.wait()
    kp, vp = pools
    me = scal[0]
    row = 2 * plan.bits
    factor = math.log2(math.e) / math.sqrt(DH)
    win = 3 * B

    def step(kk, carry):
        i = lists[row + 2, kk]
        first = (me * blk + i) == 0
        last = (me * blk + i) == plan.blocks - 1
        col = lax.broadcasted_iota(jnp.int32, (B, win), 1)
        dead = (first & (col < B)) | (last & (col >= 2 * B))
        rows = pl.ds(pl.multiple_of(i * B, B), B)
        for h in range(hd):
            qt = q[rows, h * DH : (h + 1) * DH]
            spans = [
                (pl.ds(pl.multiple_of((h * per + i) * B, B), win), win),
                (pl.ds((h * per + 2 + blk) * B, G * B), G * B),
            ]
            for r in range(R):
                at = table[i * R + r, h]
                spans.append((pl.ds(pl.multiple_of(at * B, B), B), B))
            scores = []
            for number, (span, width) in enumerate(spans):
                s = lax.dot_general(
                    qt, kp[span, :], (((1,), (1,)), ((), ())), preferred_element_type=jnp.float32
                )
                if number == 0:
                    s = jnp.where(dead, neg_big, s)
                scores.append(s)
            top = functools.reduce(
                jnp.maximum, [jnp.max(s, axis=1, keepdims=True) for s in scores]
            )
            total = jnp.zeros((B, 1), jnp.float32)
            acc = jnp.zeros((B, DH), jnp.float32)
            for s, (span, width) in zip(scores, spans):
                p = jnp.exp2((s - top) * factor)
                total = total + jnp.sum(p, axis=1, keepdims=True)
                acc = acc + jnp.dot(
                    p.astype(jnp.bfloat16), vp[span, :], preferred_element_type=jnp.float32
                )
            out[rows, h * DH : (h + 1) * DH] = (acc / total).astype(jnp.bfloat16)
        return carry

    lax.fori_loop(0, lists[row + 3, 0], step, 0)


def attend(plan, sizes, lists, table, scal, q, ins):
    count = 2 * (4 * plan.heads + plan.bits)
    return pl.pallas_call(
        functools.partial(attend_body, plan, sizes),
        out_shape=jax.ShapeDtypeStruct(q.shape, jnp.bfloat16),
        in_specs=[SMEM, SMEM, SMEM, VMEM] + [ANY] * len(ins),
        out_specs=VMEM,
        scratch_shapes=[
            pltpu.VMEM((plan.pool * B, DH), jnp.bfloat16),
            pltpu.VMEM((plan.pool * B, DH), jnp.bfloat16),
            pltpu.SemaphoreType.DMA((count,)),
        ],
        name="attend",
    )(lists, table, scal, q, *ins)


def swap(x, bit, count, down_only=False):
    pairs = [(i, i ^ bit) for i in range(count) if not down_only or i & bit]
    return lax.ppermute(x, "seq", pairs)


def body(queries, keys, values, random_holder, random_offset, keep):
    tok_dev, width_dev = queries.shape
    blk_dev = tok_dev // B
    head_dev = width_dev // DH
    count = lax.axis_size("seq")
    groups = lax.axis_size("head")
    plan = Plan(count, groups, blk_dev, head_dev)
    bits = plan.bits
    me = lax.axis_index("seq")
    scal = jnp.stack((me, lax.axis_index("head"))).astype(jnp.int32)

    ids = (random_holder * blk_dev + random_offset).reshape(head_dev, plan.req).T
    asked = jnp.where(jnp.repeat(keep, R)[:, None] > 0, ids, -1)
    mine = jnp.concatenate((asked, jnp.broadcast_to(keep[:, None], (blk_dev, head_dev))), axis=0)
    everyone = lax.all_gather(mine, ("seq", "head"), axis=1, tiled=True)
    lists, table = make_lists(plan, scal, everyone, ids)

    up = [(i, i + 1) for i in range(count - 1)]
    down = [(i + 1, i) for i in range(count - 1)]
    near = []
    for x in (keys, values):
        low = lax.ppermute(x[tok_dev - B :], "seq", up)
        high = lax.ppermute(x[:B], "seq", down)
        shared = x[: G * B]
        for s in range(bits):
            bit = count >> (s + 1)
            pairs = [(i, i + bit) for i in range(0, count, 2 * bit)]
            got = lax.ppermute(shared, "seq", pairs)
            arrives = (me & (2 * bit - 1)) == bit
            shared = jnp.where(arrives, got, shared)
        near.append((low, high, shared))

    blk_bits = log2(blk_dev)

    def fetch_and_attend(sizes):
        def run(queries, keys, values, near, lists, table, scal):
            got = ([], [])
            for s in range(bits):
                bases = [plan.own] + [plan.own + at for at in plan.base[1 : s + 1]]
                if s:
                    bases[s] = plan.own + plan.base[s]
                for which, own in enumerate((keys, values)):
                    packed = pack(
                        s, sizes[s], bases, blk_bits, lists, [own] + got[which], DH, "pack_tiles"
                    )
                    got[which].append(swap(packed, count >> (s + 1), count))
            ins = [keys, *near[0], values, *near[1], *got[0], *got[1]]
            return attend(plan, sizes, lists, table, scal, queries, ins)

        return run

    row = 2 * bits
    chosen = lists[row + 1]
    attended = lax.switch(
        chosen[0],
        [fetch_and_attend(sizes) for sizes in plan.route_sizes()],
        queries, keys, values, near, lists, table, scal,
    )

    def compact(sizes):
        def run(attended, lists):
            got = []
            for s in range(bits):
                bases = [plan.blk + at for at in plan.cbase[: s + 1]]
                packed = pack(
                    bits + s, sizes[s], bases, None, lists, [attended] + got, width_dev,
                    "pack_blocks",
                )
                got.append(swap(packed, count >> (s + 1), count, s == 0))
            bases = [plan.blk + at for at in plan.cbase + [sum(plan.cfull)]]
            return final(row, blk_dev, bases, lists, [attended] + got, width_dev)

        return run

    return lax.switch(chosen[1], [compact(sizes) for sizes in plan.pack_sizes()], attended, lists)


def solution(mesh):
    in_specs = (
        P("seq", "head"),
        P("seq", "head"),
        P("seq", "head"),
        P("head", "seq", None),
        P("head", "seq", None),
        P("seq"),
    )
    out_specs = P("seq", "head")
    return jax.shard_map(body, mesh=mesh, in_specs=in_specs, out_specs=out_specs, check_vma=False)
```

```python
import functools
import math

import jax
import jax.numpy as jnp
from jax import lax
from jax.experimental import pallas as pl
from jax.experimental.pallas import tpu as pltpu
from jax.sharding import PartitionSpec as P

DH = 128
B = 128
G = 2
R = 3
LANES = 128

neg_big = -1e30

ROUTE_SHARES = ((0.66, 0.545, 0.61), (0.73, 0.6, 0.7), (1.0, 1.0, 1.0))
PACK_SHARES = ((0.7, 0.35, 0.75), (0.8, 0.45, 0.85), (1.0, 1.0, 1.0))
PARTS = 2
SPLIT = (4, 6)


def log2(size):
    assert size & (size - 1) == 0
    return size.bit_length() - 1


class Plan:
    def __init__(self, count, groups, blk_dev, head_dev):
        self.count, self.groups, self.blk, self.heads = count, groups, blk_dev, head_dev
        self.bits = log2(count)
        self.stride = groups * head_dev
        self.lanes = count * self.stride
        self.blocks = count * blk_dev
        self.req = blk_dev * R
        self.per_head = blk_dev + 2 + G
        self.own = blk_dev * head_dev
        most = max(2, (self.req + count - 1) // count)
        bound = (count // 2) * most * head_dev
        self.full = [min(self.own << s, bound) for s in range(self.bits)]
        self.base = [sum(self.full[:s]) for s in range(self.bits)]
        self.pool = head_dev * self.per_head + sum(self.full)
        self.cfull = [
            min((blk_dev - 1) << s, blk_dev << (self.bits - 1 - s)) for s in range(self.bits)
        ]
        self.cbase = [sum(self.cfull[:s]) for s in range(self.bits)]
        self.width = -(-max(self.full + self.cfull) // LANES) * LANES

    def sizes(self, full, shares):
        out = []
        for s in range(self.bits):
            share = shares[0] if s == 0 else shares[2] if s == self.bits - 1 else shares[1]
            out.append(min(full[s], max(1, math.ceil(full[s] * share))))
        return out

    def route_sizes(self):
        return [self.sizes(self.full, shares) for shares in ROUTE_SHARES]

    def pack_sizes(self):
        return [self.sizes(self.cfull, shares) for shares in PACK_SHARES]

    def rows(self):
        return 2 * self.bits + 4


def iota(shape, axis):
    return lax.broadcasted_iota(jnp.int32, shape, axis)


def flag(cond):
    return jnp.where(cond, 1.0, 0.0)


def dot(a, b):
    return jnp.dot(
        a.astype(jnp.bfloat16), b.astype(jnp.bfloat16), preferred_element_type=jnp.float32
    )


def choose(tops, sizes):
    index = jnp.int32(len(sizes) - 1)
    for number in reversed(range(len(sizes) - 1)):
        fits = functools.reduce(
            jnp.logical_and, [top <= float(size) for top, size in zip(tops, sizes[number])]
        )
        index = jnp.where(fits, jnp.int32(number), index)
    return index


def lists_body(plan, scal, ids, own_ids, lists, table):
    me, group = scal[0], scal[1]
    T, L, hd = plan.blocks, plan.lanes, plan.heads
    lb, ls, lh = log2(plan.blk), log2(plan.stride), log2(hd)
    W = plan.width
    t = iota((T, L), 0)
    lane = iota((T, L), 1)
    holder = jnp.right_shift(lane, ls)
    need = jnp.zeros((T, L), jnp.int32)
    for k in range(plan.req):
        need = jnp.where(t == ids[k : k + 1, :], 1, need)
    near = (t >= holder * plan.blk - 1) & (t <= (holder + 1) * plan.blk)
    need = jnp.where(near | (t < G), 0, need)
    needb = need.astype(jnp.float32).astype(jnp.bfloat16)
    x = iota((L, L), 0)
    y = iota((L, L), 1)
    lower = flag(iota((T, T), 0) > iota((T, T), 1)).astype(jnp.bfloat16)
    upper = flag(iota((hd, hd), 0) < iota((hd, hd), 1)).astype(jnp.bfloat16)
    same = flag(jnp.right_shift(x, lh) == jnp.right_shift(y, lh)).astype(jnp.bfloat16)
    xe = iota((L, hd), 0)
    he = iota((L, hd), 1)
    th = iota((T, hd), 0)
    hh = iota((T, hd), 1)
    blk_of = jnp.right_shift(th, lb)
    pos_of = th & (plan.blk - 1)
    is_own = blk_of == me
    loc = jnp.where(is_own, jnp.left_shift(hh, lb) + pos_of, 0)
    slot_w = iota((T, W), 1)
    tops = []

    def order(mask):
        within = jnp.dot(lower, mask.astype(jnp.bfloat16), preferred_element_type=jnp.float32)
        cols = jnp.broadcast_to(jnp.sum(mask, axis=0, keepdims=True), (8, hd))
        return within + dot(cols, upper)[0:1, :]

    for s in range(plan.bits):
        b = plan.bits - 1 - s
        free = ((1 << b) - 1) << ls
        group_of = flag(((x ^ y) & ~free) == 0).astype(jnp.bfloat16)
        wanted = jnp.dot(needb, group_of, preferred_element_type=jnp.float32)
        into = ((jnp.right_shift(t, lb) ^ holder ^ (1 << b)) & ((2 << b) - 1)) == 0
        recv = flag((wanted > 0.5) & into)
        cols = jnp.broadcast_to(jnp.sum(recv, axis=0, keepdims=True), (8, L))
        tops.append(jnp.max(dot(cols, same)))
        recvb = recv.astype(jnp.bfloat16)
        mine = flag(xe == me * plan.stride + group * hd + he).astype(jnp.bfloat16)
        theirs = flag(xe == (me ^ (1 << b)) * plan.stride + group * hd + he).astype(jnp.bfloat16)
        got = jnp.dot(recvb, mine, preferred_element_type=jnp.float32)
        sent = jnp.dot(recvb, theirs, preferred_element_type=jnp.float32)
        place = jnp.where(sent > 0.5, order(sent).astype(jnp.int32), -1)
        line = jnp.zeros((1, W), jnp.int32)
        for h in range(hd):
            hit = place[:, h : h + 1] == slot_w
            line = line + jnp.sum(
                jnp.where(hit, loc[:, h : h + 1] + 1, 0), axis=0, keepdims=True
            )
        lists[s : s + 1, :] = line
        loc = jnp.where(
            got > 0.5, plan.own + plan.base[s] + order(got).astype(jnp.int32), loc
        )
    per = plan.per_head
    at = jnp.where(is_own, hh * per + 1 + pos_of, loc + hd * (per - plan.blk))
    at = jnp.where(th == me * plan.blk - 1, hh * per, at)
    at = jnp.where(th == (me + 1) * plan.blk, hh * per + 1 + plan.blk, at)
    at = jnp.where((th < G) & ~is_own, hh * per + 2 + plan.blk + th, at)
    for k in range(plan.req):
        hit = th == own_ids[k : k + 1, :]
        table[k : k + 1, 0:hd] = jnp.sum(jnp.where(hit, at, 0), axis=0, keepdims=True)

    kept = jnp.zeros((T, L), jnp.int32)
    head_lane = (jnp.right_shift(t, lb) == holder) & ((lane & (plan.stride - 1)) == 0)
    for i in range(plan.blk):
        hit = head_lane & ((t & (plan.blk - 1)) == i)
        kept = kept + jnp.where(hit, ids[plan.req + i : plan.req + i + 1, :], 0)
    kept = jnp.broadcast_to(jnp.sum(kept, axis=1, keepdims=True), (T, W))
    tw = iota((T, W), 0)
    dev = jnp.right_shift(tw, lb)

    def before(mask):
        return jnp.dot(
            lower, mask.astype(jnp.float32).astype(jnp.bfloat16), preferred_element_type=jnp.float32
        ).astype(jnp.int32)

    rank = before(kept)
    dest = jnp.right_shift(rank, lb)
    cloc = jnp.where(dev == me, tw & (plan.blk - 1), 0)
    ctops = []
    for s in range(plan.bits):
        b = plan.bits - 1 - s
        ok = (kept > 0) & (jnp.right_shift(dest ^ slot_w, b) == 0)
        ok = ok & (((dev ^ slot_w ^ (1 << b)) & ((2 << b) - 1)) == 0)
        recv = jnp.where(ok, 1, 0)
        ctops.append(jnp.max(jnp.sum(recv.astype(jnp.float32), axis=0, keepdims=True)))
        got = jnp.sum(jnp.where(slot_w == me, recv, 0), axis=1, keepdims=True)
        sent = jnp.sum(jnp.where(slot_w == (me ^ (1 << b)), recv, 0), axis=1, keepdims=True)
        got = jnp.broadcast_to(got, (T, W))
        sent = jnp.broadcast_to(sent, (T, W))
        hit = (sent > 0) & (before(sent) == slot_w)
        row = plan.bits + s
        lists[row : row + 1, :] = jnp.sum(jnp.where(hit, cloc + 1, 0), axis=0, keepdims=True)
        cloc = jnp.where(got > 0, plan.blk + plan.cbase[s] + before(got), cloc)
    row = 2 * plan.bits
    hit = (kept > 0) & (rank == me * plan.blk + slot_w) & (slot_w < plan.blk)
    lists[row : row + 1, :] = jnp.sum(jnp.where(hit, cloc + 1, 0), axis=0, keepdims=True)
    both = [a + c for a, c in zip(plan.route_sizes(), plan.pack_sizes())]
    lists[row + 1 : row + 2, :] = jnp.broadcast_to(choose(tops + ctops, both), (1, W))
    first = jnp.sum(jnp.where(tw < me * plan.blk, kept, 0), axis=0, keepdims=True)
    hit = (kept > 0) & (dev == me) & (rank - first == slot_w)
    lists[row + 2 : row + 3, :] = jnp.sum(
        jnp.where(hit, tw & (plan.blk - 1), 0), axis=0, keepdims=True
    )
    lists[row + 3 : row + 4, :] = jnp.sum(
        jnp.where((dev == me), kept, 0), axis=0, keepdims=True
    )


SMEM = pl.BlockSpec(memory_space=pltpu.SMEM)
VMEM = pl.BlockSpec(memory_space=pltpu.VMEM)
HBM = pl.BlockSpec(memory_space=pltpu.HBM)
ANY = pl.BlockSpec(memory_space=pl.ANY)


def make_lists(plan, scal, ids, own_ids):
    return pl.pallas_call(
        functools.partial(lists_body, plan),
        out_shape=(
            jax.ShapeDtypeStruct((plan.rows(), plan.width), jnp.int32),
            jax.ShapeDtypeStruct((plan.req, LANES), jnp.int32),
        ),
        in_specs=[SMEM, VMEM, VMEM],
        out_specs=(VMEM, VMEM),
        name="make_lists",
    )(scal, ids, own_ids)


def pack_body(row, size, bases, own_part, rows, lists, *refs):
    sources, out = refs[1:-1], refs[-1]

    def step(j, carry):
        code = jnp.maximum(lists[row, j] - 1, 0)
        target = pl.ds(pl.multiple_of(j * rows, rows), rows)

        @pl.when(code < bases[0])
        def _():
            out[target, :] = own_part(sources[0], code)

        for number, source in enumerate(sources[1:]):
            low = bases[number]

            @pl.when((code >= low) & (code < bases[number + 1]))
            def _():
                at = pl.multiple_of((code - low) * rows, rows)
                out[target, :] = source[pl.ds(at, rows), :]

        return carry

    lax.fori_loop(0, size, step, 0)


def pack(row, size, bases, own_part, rows, lists, after, sources, width, name):
    return pl.pallas_call(
        functools.partial(pack_body, row, size, bases, own_part, rows),
        out_shape=jax.ShapeDtypeStruct((size * rows, width), jnp.bfloat16),
        in_specs=[SMEM, ANY] + [VMEM] * len(sources),
        out_specs=VMEM,
        name=name,
    )(lists, after, *sources)


def either_body(after, scal, a, b, out):
    @pl.when(scal[2] == 0)
    def _():
        out[...] = a[...]

    @pl.when(scal[2] != 0)
    def _():
        out[...] = b[...]


def either(after, cond, a, b):
    return pl.pallas_call(
        either_body,
        out_shape=jax.ShapeDtypeStruct(a.shape, a.dtype),
        in_specs=[ANY, SMEM, VMEM, VMEM],
        out_specs=VMEM,
        name="either",
    )(after, cond, a, b)


def edges_body(after, keys, values, low, high, first_keys, first_values):
    tokens, width = keys.shape
    low[:, :width] = keys[tokens - B : tokens, :]
    low[:, width:] = values[tokens - B : tokens, :]
    high[:, :width] = keys[:B, :]
    high[:, width:] = values[:B, :]
    first_keys[...] = keys[: G * B, :]
    first_values[...] = values[: G * B, :]


def edges(after, keys, values):
    width, dtype = keys.shape[1], keys.dtype
    block = jax.ShapeDtypeStruct((B, 2 * width), dtype)
    shared = jax.ShapeDtypeStruct((G * B, width), dtype)
    return pl.pallas_call(
        edges_body,
        out_shape=(block, block, shared, shared),
        in_specs=[ANY, VMEM, VMEM],
        out_specs=(VMEM,) * 4,
        name="edges",
    )(after, keys, values)


def hold_body(after, before, x, out):
    pass


def hold(after, before, x):
    return pl.pallas_call(
        hold_body,
        out_shape=jax.ShapeDtypeStruct(x.shape, x.dtype),
        in_specs=[ANY, ANY, ANY],
        out_specs=ANY,
        input_output_aliases={2: 0},
        name="hold",
    )(after, before, x)


def tile_part(heads_bits, part, rows):
    def read(own, code):
        head = jnp.right_shift(code, heads_bits)
        pos = code & ((1 << heads_bits) - 1)
        at = pl.multiple_of(pos * B + part * rows, rows)
        return own[pl.ds(at, rows), pl.ds(pl.multiple_of(head * DH, DH), DH)]

    return read


def block_part(own, code):
    return own[pl.ds(pl.multiple_of(code * B, B), B), :]


def final_body(row, slots, bases, widths, lists, *refs):
    out = refs[-1]
    per = (len(refs) - 1) // len(widths)

    def step(j, carry):
        code = lists[row, j]
        target = pl.ds(pl.multiple_of(j * B, B), B)

        @pl.when(code == 0)
        def _():
            out[target, :] = jnp.zeros((B, out.shape[1]), out.dtype)

        for number in range(per):
            low = 0 if number == 0 else bases[number - 1]

            @pl.when((code - 1 >= low) & (code - 1 < bases[number]))
            def _():
                at = pl.multiple_of((code - 1 - low) * B, B)
                for part, width in enumerate(widths):
                    first = sum(widths[:part])
                    out[target, first : first + width] = refs[part * per + number][
                        pl.ds(at, B), :
                    ]

        return carry

    lax.fori_loop(0, slots, step, 0)


def final(row, slots, bases, lists, sources, widths):
    return pl.pallas_call(
        functools.partial(final_body, row, slots, bases, widths),
        out_shape=jax.ShapeDtypeStruct((slots * B, sum(widths)), jnp.bfloat16),
        in_specs=[SMEM] + [VMEM] * len(sources),
        out_specs=VMEM,
        name="place_blocks",
    )(lists, *sources)


FACTOR = math.log2(math.e) / math.sqrt(DH)


def scores_of(qt, kt):
    return lax.dot_general(
        qt, kt, (((1,), (1,)), ((), ())), preferred_element_type=jnp.float32
    )


def gather_parts(scores, values, top):
    total = 0.0
    acc = 0.0
    for s, vt in zip(scores, values):
        p = jnp.exp2((s - top) * FACTOR)
        total = total + jnp.sum(p, axis=1, keepdims=True)
        acc = acc + jnp.dot(p.astype(jnp.bfloat16), vt, preferred_element_type=jnp.float32)
    return total, acc


def peak(scores):
    return functools.reduce(jnp.maximum, [jnp.max(s, axis=1, keepdims=True) for s in scores])


def start_near(plan, heads, own, low, high, shared, first, pool, sem, copies):
    wide = plan.heads * DH
    for h in heads:
        cols = pl.ds(h * DH, DH)
        there = pl.ds(first * wide + h * DH, DH)
        for source, at, tiles in (
            (low.at[:, there], 0, 1),
            (own.at[:, cols], 1, plan.blk),
            (high.at[:, there], 1 + plan.blk, 1),
            (shared.at[:, cols], 2 + plan.blk, G),
        ):
            copy = pltpu.make_async_copy(
                source,
                pool.at[pl.ds((h * plan.per_head + at) * B, tiles * B), :],
                sem.at[len(copies)],
            )
            copy.start()
            copies.append(copy)


def start_far(plan, sizes, chunks, pool, sem, copies):
    rows = B // PARTS
    for part in range(PARTS):
        for s in range(plan.bits):
            copy = pltpu.make_async_copy(
                chunks[part * plan.bits + s],
                pool.at[pl.ds(plan.base[s], sizes[s]), pl.ds(part * rows, rows), :],
                sem.at[len(copies)],
            )
            copy.start()
            copies.append(copy)


def tile_reader(plan, near_pool, far_pool, at):
    split = plan.heads * plan.per_head
    inside = at < split
    row = pl.multiple_of(jnp.where(inside, at, 0) * B, B)
    near = near_pool[pl.ds(row, B), :]
    far = far_pool[jnp.where(inside, 0, at - split)]
    return jnp.where(inside, near, far)


def put_stats(stat, rows, hd, h, top, total):
    lane = lax.broadcasted_iota(jnp.int32, (B, LANES), 1)
    old = stat[rows, :]
    stat[rows, :] = jnp.where(lane == h, top, jnp.where(lane == hd + h, total, old))


def near_body(plan, lists, scal, after, q, *refs):
    k, v, low, high, shared_k, shared_v, acc_out, stat_out, kp, vp, sem = refs
    blk, hd, per = plan.blk, plan.heads, plan.per_head
    copies = []
    start_near(plan, range(hd), k, low, high, shared_k, 0, kp, sem, copies)
    start_near(plan, range(hd), v, low, high, shared_v, 1, vp, sem, copies)
    for copy in copies:
        copy.wait()
    me = scal[0]
    row = 2 * plan.bits
    win = 3 * B

    def step(kk, carry):
        i = lists[row + 2, kk]
        first = (me * blk + i) == 0
        last = (me * blk + i) == plan.blocks - 1
        col = lax.broadcasted_iota(jnp.int32, (B, win), 1)
        dead = (first & (col < B)) | (last & (col >= 2 * B))
        rows = pl.ds(pl.multiple_of(i * B, B), B)
        for h in range(hd):
            qt = q[rows, h * DH : (h + 1) * DH]
            spans = (
                pl.ds(pl.multiple_of((h * per + i) * B, B), win),
                pl.ds((h * per + 2 + blk) * B, G * B),
            )
            scores = [scores_of(qt, kp[span, :]) for span in spans]
            scores[0] = jnp.where(dead, neg_big, scores[0])
            top = peak(scores)
            total, acc = gather_parts(scores, [vp[span, :] for span in spans], top)
            acc_out[rows, h * DH : (h + 1) * DH] = acc
            stat_out[rows, h : h + 1] = top
            stat_out[rows, hd + h : hd + h + 1] = total
        return carry

    lax.fori_loop(0, lists[row + 3, 0], step, 0)


def near_attend(plan, lists, scal, after, q, ins):
    pool = plan.heads * plan.per_head * B
    return pl.pallas_call(
        functools.partial(near_body, plan),
        out_shape=(
            jax.ShapeDtypeStruct(q.shape, jnp.float32),
            jax.ShapeDtypeStruct((q.shape[0], LANES), jnp.float32),
        ),
        in_specs=[SMEM, SMEM, ANY, VMEM] + [HBM] * len(ins),
        out_specs=(VMEM, VMEM),
        scratch_shapes=[
            pltpu.VMEM((pool, DH), jnp.bfloat16),
            pltpu.VMEM((pool, DH), jnp.bfloat16),
            pltpu.SemaphoreType.DMA((8 * plan.heads,)),
        ],
        name="near_attend",
    )(lists, scal, after, q, *ins)


def far_scores_body(plan, sizes, lists, table, after, q, k, low, high, shared, *refs):
    count = PARTS * plan.bits
    chunks, (p_out, stat_out), (near, far, sem) = refs[:count], refs[count : count + 2], refs[count + 2 :]
    hd = plan.heads
    copies = []
    start_far(plan, sizes, chunks, far, sem, copies)
    start_near(plan, range(hd), k, low, high, shared, 0, near, sem, copies)
    for copy in copies:
        copy.wait()
    row = 2 * plan.bits

    def step(kk, carry):
        i = lists[row + 2, kk]
        rows = pl.ds(pl.multiple_of(i * B, B), B)
        for h in range(hd):
            qt = q[rows, h * DH : (h + 1) * DH]
            scores = [
                scores_of(qt, tile_reader(plan, near, far, table[i * R + r, h])) for r in range(R)
            ]
            top = peak(scores)
            total = 0.0
            for r, s in enumerate(scores):
                p = jnp.exp2((s - top) * FACTOR)
                total = total + jnp.sum(p, axis=1, keepdims=True)
                p_out[rows, (h * R + r) * B : (h * R + r + 1) * B] = p.astype(jnp.bfloat16)
            stat_out[rows, h : h + 1] = top
            stat_out[rows, hd + h : hd + h + 1] = total
        return carry

    lax.fori_loop(0, lists[row + 3, 0], step, 0)


def pools_of(plan):
    return [
        pltpu.VMEM((plan.heads * plan.per_head * B, DH), jnp.bfloat16),
        pltpu.VMEM((sum(plan.full), B, DH), jnp.bfloat16),
        pltpu.SemaphoreType.DMA((4 * plan.heads + PARTS * plan.bits,)),
    ]


def far_scores(plan, sizes, lists, table, after, q, k, low, high, shared, chunks):
    return pl.pallas_call(
        functools.partial(far_scores_body, plan, sizes),
        out_shape=(
            jax.ShapeDtypeStruct((q.shape[0], plan.heads * R * B), jnp.bfloat16),
            jax.ShapeDtypeStruct((q.shape[0], LANES), jnp.float32),
        ),
        in_specs=[SMEM, SMEM, ANY, VMEM] + [HBM] * (4 + len(chunks)),
        out_specs=(VMEM, VMEM),
        scratch_shapes=pools_of(plan),
        name="far_scores",
    )(lists, table, after, q, k, low, high, shared, *chunks)


def far_values_body(plan, sizes, heads, lists, table, after, p, pstat, acc_in, stat, v, low, high,
                    shared, *refs):
    count = PARTS * plan.bits
    chunks, out, (near, far, sem) = refs[:count], refs[count], refs[count + 1 :]
    hd = plan.heads
    copies = []
    start_far(plan, sizes, chunks, far, sem, copies)
    start_near(plan, heads, v, low, high, shared, 1, near, sem, copies)
    for copy in copies:
        copy.wait()
    row = 2 * plan.bits

    def step(kk, carry):
        i = lists[row + 2, kk]
        rows = pl.ds(pl.multiple_of(i * B, B), B)
        for number, h in enumerate(heads):
            acc = 0.0
            for r in range(R):
                acc = acc + jnp.dot(
                    p[rows, (number * R + r) * B : (number * R + r + 1) * B],
                    tile_reader(plan, near, far, table[i * R + r, h]),
                    preferred_element_type=jnp.float32,
                )
            far_top, near_top = pstat[rows, h : h + 1], stat[rows, h : h + 1]
            top = jnp.maximum(far_top, near_top)
            a = jnp.exp2((far_top - top) * FACTOR)
            c = jnp.exp2((near_top - top) * FACTOR)
            total = a * pstat[rows, hd + h : hd + h + 1] + c * stat[rows, hd + h : hd + h + 1]
            scale = 1.0 / total
            acc = (a * scale) * acc + (c * scale) * acc_in[rows, number * DH : (number + 1) * DH]
            out[rows, number * DH : (number + 1) * DH] = acc.astype(jnp.bfloat16)
        return carry

    lax.fori_loop(0, lists[row + 3, 0], step, 0)


def far_values(plan, sizes, heads, lists, table, after, p, pstat, acc, stat, v, low, high, shared,
               chunks):
    size = len(heads)
    assert heads[0] % size == 0

    def of_team(x, width):
        return pl.BlockSpec((x.shape[0], size * width), lambda _: (0, heads[0] // size))

    return pl.pallas_call(
        functools.partial(far_values_body, plan, sizes, heads),
        out_shape=jax.ShapeDtypeStruct((p.shape[0], len(heads) * DH), jnp.bfloat16),
        grid=(1,),
        in_specs=[SMEM, SMEM, ANY, of_team(p, R * B), VMEM, of_team(acc, DH), VMEM]
        + [HBM] * (4 + len(chunks)),
        out_specs=VMEM,
        scratch_shapes=pools_of(plan),
        name="far_values",
    )(lists, table, after, p, pstat, acc, stat, v, low, high, shared, *chunks)


def swap(x, bit, count, down_only=False):
    pairs = [(i, i ^ bit) for i in range(count) if not down_only or i & bit]
    return lax.ppermute(x, "seq", pairs)


def body(queries, keys, values, random_holder, random_offset, keep):
    tok_dev, width_dev = queries.shape
    blk_dev = tok_dev // B
    head_dev = width_dev // DH
    count = lax.axis_size("seq")
    groups = lax.axis_size("head")
    plan = Plan(count, groups, blk_dev, head_dev)
    bits = plan.bits
    me = lax.axis_index("seq")
    scal = jnp.stack((me, lax.axis_index("head"))).astype(jnp.int32)

    ids = (random_holder * blk_dev + random_offset).reshape(head_dev, plan.req).T
    asked = jnp.where(jnp.repeat(keep, R)[:, None] > 0, ids, -1)
    mine = jnp.concatenate((asked, jnp.broadcast_to(keep[:, None], (blk_dev, head_dev))), axis=0)
    everyone = lax.all_to_all(
        jnp.broadcast_to(mine[None], (count * groups,) + mine.shape),
        ("seq", "head"), split_axis=0, concat_axis=0, tiled=True,
    )
    everyone = jnp.transpose(everyone, (1, 0, 2)).reshape(mine.shape[0], plan.lanes)
    lists, table = make_lists(plan, scal, everyone, ids)

    blk_bits = log2(blk_dev)
    rows = B // PARTS
    row = 2 * bits
    cuts = [0] + [cut for cut in SPLIT if cut < head_dev] + [head_dev]
    if len(cuts) == 2:
        cuts = [0, head_dev // 2, head_dev]
    teams = [range(low, high) for low, high in zip(cuts, cuts[1:])]
    flags = lambda cond: jnp.concatenate((scal, cond.astype(jnp.int32)[None]))
    odd = flags((me & 1) == 1)

    def branch(sizes, csizes):
        def run(queries, keys, values, lists, table, scal, odd):
            got = [[] for _ in range(2 * PARTS)]
            last = [lists]

            def run_after(fn, *args):
                out = fn(last[0], *args)
                last[0] = out[0] if isinstance(out, (tuple, list)) else out
                return out

            def packed_tiles(s, chunk):
                which, part = chunk // PARTS, chunk % PARTS
                bases = [plan.own + at for at in plan.base[: s + 1]]
                return run_after(
                    lambda after: pack(
                        s, sizes[s], bases, tile_part(blk_bits, part, rows), rows, lists, after,
                        [(keys, values)[which]] + got[chunk], DH, "pack_tiles",
                    )
                )

            def stage(s, chunk):
                got[chunk].append(swap(packed_tiles(s, chunk), count >> (s + 1), count))

            def tiles(which):
                return [
                    x.reshape(-1, rows, DH)
                    for part in range(PARTS)
                    for x in got[which * PARTS + part]
                ]

            def begin(chunk, packed):
                packed = run_after(lambda after: hold(after, got[chunk - 1][0], packed))
                got[chunk].append(swap(packed, count >> 1, count))

            def hop(x, pairs):
                return lax.ppermute(x, "seq", pairs)

            stage(0, 0)
            low, high, first_keys, first_values = run_after(edges, keys, values)
            low = hop(low, [(i, i + 1) for i in range(count - 1)])
            high = hop(high, [(i + 1, i) for i in range(count - 1)])
            beside = hop(first_values, [(0, 1)])
            coming = packed_tiles(0, 1)
            held = run_after(either, odd, first_keys, beside)
            spreads = []
            for s in range(bits - 1):
                bit = count >> (s + 1)
                spreads.append(
                    (bit, [(i + j, i + j + bit) for i in range(0, count, 2 * bit) for j in (0, 1)])
                )
            chunks = 2 * PARTS
            for step in range(chunks + bits - 1):
                there = None
                if step < len(spreads):
                    bit, pairs = spreads[step]
                    there = hop(held, pairs)
                elif step == len(spreads):
                    there = swap(held, 1, count)
                if step + 1 < chunks:
                    begin(step + 1, coming)
                for s in range(1, bits):
                    if 0 <= step + 1 - s < chunks:
                        stage(s, step + 1 - s)
                    if s == 1 and step + 2 < chunks:
                        coming = packed_tiles(0, step + 2)
                if step < len(spreads):
                    held = run_after(either, flags((me & bit) != 0), held, there)
                elif step == len(spreads):
                    shared_keys = run_after(either, odd, held, there)
                    shared_values = run_after(either, odd, there, held)
                if step == max(len(spreads), chunks - 2):
                    acc, stat = run_after(
                        lambda after: near_attend(
                            plan, lists, scal, after, queries,
                            [keys, values, low, high, shared_keys, shared_values],
                        )
                    )
                if step == chunks + bits - 3:
                    p, pstat = run_after(
                        lambda after: far_scores(
                            plan, sizes, lists, table, after, queries, keys, low, high,
                            shared_keys, tiles(0),
                        )
                    )

            sources = []

            def pack_stage(s, held):
                bases = [plan.blk + at for at in plan.cbase[: s + 1]]
                packed = run_after(
                    lambda after: pack(
                        bits + s, csizes[s], bases, block_part, B, lists, after, held,
                        held[0].shape[1], "pack_blocks",
                    )
                )
                held.append(swap(packed, count >> (s + 1), count, s == 0))

            for half, heads in enumerate(teams):
                attended = run_after(
                    lambda after: far_values(
                        plan, sizes, heads, lists, table, after, p, pstat, acc, stat, values,
                        low, high, shared_values, tiles(1),
                    )
                )
                sources.append([attended])
                pack_stage(0, sources[half])
            for step in range(len(teams) + bits - 2):
                for s in range(1, bits):
                    if 0 <= step + 1 - s < len(teams):
                        pack_stage(s, sources[step + 1 - s])
            bases = [plan.blk + at for at in plan.cbase + [sum(plan.cfull)]]
            widths = [len(heads) * DH for heads in teams]
            return final(row, blk_dev, bases, lists, sum(sources, []), widths)

        return run

    return lax.switch(
        lists[row + 1, 0],
        [branch(a, c) for a, c in zip(plan.route_sizes(), plan.pack_sizes())],
        queries, keys, values, lists, table, scal, odd,
    )


def solution(mesh):
    in_specs = (
        P("seq", "head"),
        P("seq", "head"),
        P("seq", "head"),
        P("head", "seq", None),
        P("head", "seq", None),
        P("seq"),
    )
    out_specs = P("seq", "head")
    return jax.shard_map(body, mesh=mesh, in_specs=in_specs, out_specs=out_specs, check_vma=False)
```

```python
import functools
import math

import jax
import jax.numpy as jnp
from jax import lax
from jax.experimental import pallas as pl
from jax.experimental.pallas import tpu as pltpu
from jax.sharding import PartitionSpec as P


DH = 128
B = 128
G = 2
R = 3
LANES = 128

neg_big = -1e30

ROUTE_SHARES = ((0.66, 0.545, 0.61), (0.73, 0.6, 0.7), (1.0, 1.0, 1.0))
PACK_SHARES = ((0.7, 0.35, 0.75), (0.8, 0.45, 0.85), (1.0, 1.0, 1.0))
PARTS = 2
UNROLL = 4
SPLIT = (2, 4, 6)


def log2(size):
    assert size & (size - 1) == 0
    return size.bit_length() - 1


class Plan:
    def __init__(self, count, groups, blk_dev, head_dev):
        self.count, self.groups, self.blk, self.heads = count, groups, blk_dev, head_dev
        self.bits = log2(count)
        self.stride = groups * head_dev
        self.lanes = count * self.stride
        self.blocks = count * blk_dev
        self.req = blk_dev * R
        self.per_head = blk_dev + 2 + G
        self.own = blk_dev * head_dev
        most = max(2, (self.req + count - 1) // count)
        bound = (count // 2) * most * head_dev
        self.full = [min(self.own << s, bound) for s in range(self.bits)]
        self.base = [sum(self.full[:s]) for s in range(self.bits)]
        self.cfull = [
            min((blk_dev - 1) << s, blk_dev << (self.bits - 1 - s)) for s in range(self.bits)
        ]
        self.cbase = [sum(self.cfull[:s]) for s in range(self.bits)]
        self.width = -(-max(self.full + self.cfull) // LANES) * LANES

    def sizes(self, full, shares):
        out = []
        for s in range(self.bits):
            share = shares[0] if s == 0 else shares[2] if s == self.bits - 1 else shares[1]
            out.append(min(full[s], max(1, math.ceil(full[s] * share))))
        return out

    def route_sizes(self):
        return [self.sizes(self.full, shares) for shares in ROUTE_SHARES]

    def pack_sizes(self):
        return [self.sizes(self.cfull, shares) for shares in PACK_SHARES]

    def rows(self):
        return 2 * self.bits + 4


def iota(shape, axis):
    return lax.broadcasted_iota(jnp.int32, shape, axis)


def flag(cond):
    return jnp.where(cond, 1.0, 0.0)


def dot(a, b):
    return jnp.dot(
        a.astype(jnp.bfloat16), b.astype(jnp.bfloat16), preferred_element_type=jnp.float32
    )


def choose(tops, sizes):
    index = jnp.int32(len(sizes) - 1)
    for number in reversed(range(len(sizes) - 1)):
        fits = functools.reduce(
            jnp.logical_and, [top <= float(size) for top, size in zip(tops, sizes[number])]
        )
        index = jnp.where(fits, jnp.int32(number), index)
    return index


def lists_body(plan, scal, ids, own_ids, lists, table):
    me, group = scal[0], scal[1]
    T, L, hd = plan.blocks, plan.lanes, plan.heads
    lb, ls, lh = log2(plan.blk), log2(plan.stride), log2(hd)
    W = plan.width
    t = iota((T, L), 0)
    lane = iota((T, L), 1)
    holder = jnp.right_shift(lane, ls)
    need = jnp.zeros((T, L), jnp.int32)
    for k in range(plan.req):
        need = jnp.where(t == ids[k : k + 1, :], 1, need)
    near = (t >= holder * plan.blk - 1) & (t <= (holder + 1) * plan.blk)
    need = jnp.where(near | (t < G), 0, need)
    needb = need.astype(jnp.float32).astype(jnp.bfloat16)
    x = iota((L, L), 0)
    y = iota((L, L), 1)
    lower = flag(iota((T, T), 0) > iota((T, T), 1)).astype(jnp.bfloat16)
    upper = flag(iota((hd, hd), 0) < iota((hd, hd), 1)).astype(jnp.bfloat16)
    same = flag(jnp.right_shift(x, lh) == jnp.right_shift(y, lh)).astype(jnp.bfloat16)
    xe = iota((L, hd), 0)
    he = iota((L, hd), 1)
    th = iota((T, hd), 0)
    hh = iota((T, hd), 1)
    blk_of = jnp.right_shift(th, lb)
    pos_of = th & (plan.blk - 1)
    is_own = blk_of == me
    loc = jnp.where(is_own, jnp.left_shift(hh, lb) + pos_of, 0)
    slot_w = iota((T, W), 1)
    tops = []

    def order(mask):
        within = jnp.dot(lower, mask.astype(jnp.bfloat16), preferred_element_type=jnp.float32)
        cols = jnp.broadcast_to(jnp.sum(mask, axis=0, keepdims=True), (8, hd))
        return within + dot(cols, upper)[0:1, :]

    for s in range(plan.bits):
        b = plan.bits - 1 - s
        free = ((1 << b) - 1) << ls
        group_of = flag(((x ^ y) & ~free) == 0).astype(jnp.bfloat16)
        wanted = jnp.dot(needb, group_of, preferred_element_type=jnp.float32)
        into = ((jnp.right_shift(t, lb) ^ holder ^ (1 << b)) & ((2 << b) - 1)) == 0
        recv = flag((wanted > 0.5) & into)
        cols = jnp.broadcast_to(jnp.sum(recv, axis=0, keepdims=True), (8, L))
        tops.append(jnp.max(dot(cols, same)))
        recvb = recv.astype(jnp.bfloat16)
        mine = flag(xe == me * plan.stride + group * hd + he).astype(jnp.bfloat16)
        theirs = flag(xe == (me ^ (1 << b)) * plan.stride + group * hd + he).astype(jnp.bfloat16)
        got = jnp.dot(recvb, mine, preferred_element_type=jnp.float32)
        sent = jnp.dot(recvb, theirs, preferred_element_type=jnp.float32)
        place = jnp.where(sent > 0.5, order(sent).astype(jnp.int32), -1)
        line = jnp.zeros((1, W), jnp.int32)
        for h in range(hd):
            hit = place[:, h : h + 1] == slot_w
            line = line + jnp.sum(
                jnp.where(hit, loc[:, h : h + 1] + 1, 0), axis=0, keepdims=True
            )
        lists[s : s + 1, :] = line
        loc = jnp.where(
            got > 0.5, plan.own + plan.base[s] + order(got).astype(jnp.int32), loc
        )
    per = plan.per_head
    at = jnp.where(is_own, hh * per + 1 + pos_of, loc + hd * (per - plan.blk))
    at = jnp.where(th == me * plan.blk - 1, hh * per, at)
    at = jnp.where(th == (me + 1) * plan.blk, hh * per + 1 + plan.blk, at)
    at = jnp.where((th < G) & ~is_own, hh * per + 2 + plan.blk + th, at)
    for k in range(plan.req):
        hit = th == own_ids[k : k + 1, :]
        table[k : k + 1, 0:hd] = jnp.sum(jnp.where(hit, at, 0), axis=0, keepdims=True)

    kept = jnp.zeros((T, L), jnp.int32)
    head_lane = (jnp.right_shift(t, lb) == holder) & ((lane & (plan.stride - 1)) == 0)
    for i in range(plan.blk):
        hit = head_lane & ((t & (plan.blk - 1)) == i)
        kept = kept + jnp.where(hit, ids[plan.req + i : plan.req + i + 1, :], 0)
    kept = jnp.broadcast_to(jnp.sum(kept, axis=1, keepdims=True), (T, W))
    tw = iota((T, W), 0)
    dev = jnp.right_shift(tw, lb)

    def before(mask):
        return jnp.dot(
            lower, mask.astype(jnp.float32).astype(jnp.bfloat16), preferred_element_type=jnp.float32
        ).astype(jnp.int32)

    rank = before(kept)
    dest = jnp.right_shift(rank, lb)
    cloc = jnp.where(dev == me, tw & (plan.blk - 1), 0)
    ctops = []
    for s in range(plan.bits):
        b = plan.bits - 1 - s
        ok = (kept > 0) & (jnp.right_shift(dest ^ slot_w, b) == 0)
        ok = ok & (((dev ^ slot_w ^ (1 << b)) & ((2 << b) - 1)) == 0)
        recv = jnp.where(ok, 1, 0)
        ctops.append(jnp.max(jnp.sum(recv.astype(jnp.float32), axis=0, keepdims=True)))
        got = jnp.sum(jnp.where(slot_w == me, recv, 0), axis=1, keepdims=True)
        sent = jnp.sum(jnp.where(slot_w == (me ^ (1 << b)), recv, 0), axis=1, keepdims=True)
        got = jnp.broadcast_to(got, (T, W))
        sent = jnp.broadcast_to(sent, (T, W))
        hit = (sent > 0) & (before(sent) == slot_w)
        row = plan.bits + s
        lists[row : row + 1, :] = jnp.sum(jnp.where(hit, cloc + 1, 0), axis=0, keepdims=True)
        cloc = jnp.where(got > 0, plan.blk + plan.cbase[s] + before(got), cloc)
    row = 2 * plan.bits
    hit = (kept > 0) & (rank == me * plan.blk + slot_w) & (slot_w < plan.blk)
    lists[row : row + 1, :] = jnp.sum(jnp.where(hit, cloc + 1, 0), axis=0, keepdims=True)
    both = [a + c for a, c in zip(plan.route_sizes(), plan.pack_sizes())]
    lists[row + 1 : row + 2, :] = jnp.broadcast_to(choose(tops + ctops, both), (1, W))
    first = jnp.sum(jnp.where(tw < me * plan.blk, kept, 0), axis=0, keepdims=True)
    hit = (kept > 0) & (dev == me) & (rank - first == slot_w)
    lists[row + 2 : row + 3, :] = jnp.sum(
        jnp.where(hit, tw & (plan.blk - 1), 0), axis=0, keepdims=True
    )
    lists[row + 3 : row + 4, :] = jnp.sum(
        jnp.where((dev == me), kept, 0), axis=0, keepdims=True
    )


SMEM = pl.BlockSpec(memory_space=pltpu.SMEM)
VMEM = pl.BlockSpec(memory_space=pltpu.VMEM)
HBM = pl.BlockSpec(memory_space=pltpu.HBM)
ANY = pl.BlockSpec(memory_space=pl.ANY)


def make_lists(plan, scal, ids, own_ids):
    return pl.pallas_call(
        functools.partial(lists_body, plan),
        out_shape=(
            jax.ShapeDtypeStruct((plan.rows(), plan.width), jnp.int32),
            jax.ShapeDtypeStruct((plan.req, LANES), jnp.int32),
        ),
        in_specs=[SMEM, VMEM, VMEM],
        out_specs=(VMEM, VMEM),
        name="make_lists",
    )(scal, ids, own_ids)


def pack_body(row, size, bases, own_part, rows, lists, *refs):
    sources, out = refs[1:-1], refs[-1]

    def step(j, carry):
        code = jnp.maximum(lists[row, j] - 1, 0)
        target = pl.ds(pl.multiple_of(j * rows, rows), rows)

        @pl.when(code < bases[0])
        def _():
            out[target, :] = own_part(sources[0], code)

        for number, source in enumerate(sources[1:]):
            low = bases[number]

            @pl.when((code >= low) & (code < bases[number + 1]))
            def _():
                at = pl.multiple_of((code - low) * rows, rows)
                out[target, :] = source[pl.ds(at, rows), :]

        return carry

    lax.fori_loop(0, size, step, 0)


def pack(row, size, bases, own_part, rows, lists, after, sources, width):
    return pl.pallas_call(
        functools.partial(pack_body, row, size, bases, own_part, rows),
        out_shape=jax.ShapeDtypeStruct((size * rows, width), jnp.bfloat16),
        in_specs=[SMEM, ANY] + [VMEM] * len(sources),
        out_specs=VMEM,
    )(lists, after, *sources)


def either_body(after, scal, a, b, out):
    @pl.when(scal[2] == 0)
    def _():
        out[...] = a[...]

    @pl.when(scal[2] != 0)
    def _():
        out[...] = b[...]


def either(after, cond, a, b):
    return pl.pallas_call(
        either_body,
        out_shape=jax.ShapeDtypeStruct(a.shape, a.dtype),
        in_specs=[ANY, SMEM, VMEM, VMEM],
        out_specs=VMEM,
        name="either",
    )(after, cond, a, b)


def edges_body(after, keys, values, low, high, first_keys, first_values):
    tokens, width = keys.shape
    low[:, :width] = keys[tokens - B : tokens, :]
    low[:, width:] = values[tokens - B : tokens, :]
    high[:, :width] = keys[:B, :]
    high[:, width:] = values[:B, :]
    first_keys[...] = keys[: G * B, :]
    first_values[...] = values[: G * B, :]


def edges(after, keys, values):
    width, dtype = keys.shape[1], keys.dtype
    block = jax.ShapeDtypeStruct((B, 2 * width), dtype)
    shared = jax.ShapeDtypeStruct((G * B, width), dtype)
    return pl.pallas_call(
        edges_body,
        out_shape=(block, block, shared, shared),
        in_specs=[ANY, VMEM, VMEM],
        out_specs=(VMEM,) * 4,
        name="edges",
    )(after, keys, values)


def hold_body(after, before, x, out):
    pass


def hold(after, before, x):
    return pl.pallas_call(
        hold_body,
        out_shape=jax.ShapeDtypeStruct(x.shape, x.dtype),
        in_specs=[ANY, ANY, ANY],
        out_specs=ANY,
        input_output_aliases={2: 0},
        name="hold",
    )(after, before, x)


def tile_part(heads_bits, part, rows):
    def read(own, code):
        head = jnp.right_shift(code, heads_bits)
        pos = code & ((1 << heads_bits) - 1)
        at = pl.multiple_of(pos * B + part * rows, rows)
        return own[pl.ds(at, rows), pl.ds(pl.multiple_of(head * DH, DH), DH)]

    return read


def block_part(own, code):
    return own[pl.ds(pl.multiple_of(code * B, B), B), :]


def final_body(row, slots, bases, widths, lists, *refs):
    out = refs[-1]
    per = (len(refs) - 1) // len(widths)

    def step(j, carry):
        code = lists[row, j]
        target = pl.ds(pl.multiple_of(j * B, B), B)

        @pl.when(code == 0)
        def _():
            out[target, :] = jnp.zeros((B, out.shape[1]), out.dtype)

        for number in range(per):
            low = 0 if number == 0 else bases[number - 1]

            @pl.when((code - 1 >= low) & (code - 1 < bases[number]))
            def _():
                at = pl.multiple_of((code - 1 - low) * B, B)
                for part, width in enumerate(widths):
                    first = sum(widths[:part])
                    out[target, first : first + width] = refs[part * per + number][
                        pl.ds(at, B), :
                    ]

        return carry

    lax.fori_loop(0, slots, step, 0)


def final(row, slots, bases, lists, sources, widths):
    return pl.pallas_call(
        functools.partial(final_body, row, slots, bases, widths),
        out_shape=jax.ShapeDtypeStruct((slots * B, sum(widths)), jnp.bfloat16),
        in_specs=[SMEM] + [VMEM] * len(sources),
        out_specs=VMEM,
        name="place_blocks",
    )(lists, *sources)


FACTOR = math.log2(math.e) / math.sqrt(DH)


def scores_of(qt, kt):
    return lax.dot_general(
        qt, kt, (((1,), (1,)), ((), ())), preferred_element_type=jnp.float32
    )


def gather_parts(scores, values, top):
    total = 0.0
    acc = 0.0
    for s, vt in zip(scores, values):
        p = jnp.exp2((s - top) * FACTOR)
        total = total + jnp.sum(p, axis=1, keepdims=True)
        acc = acc + jnp.dot(p.astype(jnp.bfloat16), vt, preferred_element_type=jnp.float32)
    return total, acc


def peak(scores):
    return functools.reduce(jnp.maximum, [jnp.max(s, axis=1, keepdims=True) for s in scores])


def start_near(plan, heads, own, low, high, shared, first, pool, sem, copies):
    wide = plan.heads * DH
    for h in heads:
        cols = pl.ds(h * DH, DH)
        there = pl.ds(first * wide + h * DH, DH)
        for source, at, tiles in (
            (low.at[:, there], 0, 1),
            (own.at[:, cols], 1, plan.blk),
            (high.at[:, there], 1 + plan.blk, 1),
            (shared.at[:, cols], 2 + plan.blk, G),
        ):
            copy = pltpu.make_async_copy(
                source,
                pool.at[pl.ds((h * plan.per_head + at) * B, tiles * B), :],
                sem.at[len(copies)],
            )
            copy.start()
            copies.append(copy)


def start_far(plan, sizes, chunks, pool, sem, copies):
    rows = B // PARTS
    for part in range(PARTS):
        for s in range(plan.bits):
            copy = pltpu.make_async_copy(
                chunks[part * plan.bits + s],
                pool.at[pl.ds(plan.base[s], sizes[s]), pl.ds(part * rows, rows), :],
                sem.at[len(copies)],
            )
            copy.start()
            copies.append(copy)


def tile_reader(plan, near_pool, far_pool, at):
    split = plan.heads * plan.per_head
    inside = at < split
    row = pl.multiple_of(jnp.where(inside, at, 0) * B, B)
    near = near_pool[pl.ds(row, B), :]
    far = far_pool[jnp.where(inside, 0, at - split)]
    return jnp.where(inside, near, far)


def put_stats(stat, rows, hd, h, top, total):
    lane = lax.broadcasted_iota(jnp.int32, (B, LANES), 1)
    old = stat[rows, :]
    stat[rows, :] = jnp.where(lane == h, top, jnp.where(lane == hd + h, total, old))


def near_body(plan, heads, lists, scal, after, q, *refs):
    k, v, low, high, shared_k, shared_v, acc_out, stat_out, kp, vp, sem = refs
    blk, hd, per = plan.blk, plan.heads, plan.per_head
    copies = []
    start_near(plan, heads, k, low, high, shared_k, 0, kp, sem, copies)
    start_near(plan, heads, v, low, high, shared_v, 1, vp, sem, copies)
    for copy in copies:
        copy.wait()
    me = scal[0]
    row = 2 * plan.bits
    win = 3 * B

    def step(kk, carry):
        i = lists[row + 2, kk]
        first = (me * blk + i) == 0
        last = (me * blk + i) == plan.blocks - 1
        col = lax.broadcasted_iota(jnp.int32, (B, win), 1)
        dead = (first & (col < B)) | (last & (col >= 2 * B))
        rows = pl.ds(pl.multiple_of(i * B, B), B)
        for number, h in enumerate(heads):
            qt = q[rows, h * DH : (h + 1) * DH]
            spans = (
                pl.ds(pl.multiple_of((h * per + i) * B, B), win),
                pl.ds((h * per + 2 + blk) * B, G * B),
            )
            scores = [scores_of(qt, kp[span, :]) for span in spans]
            scores[0] = jnp.where(dead, neg_big, scores[0])
            top = peak(scores)
            total, acc = gather_parts(scores, [vp[span, :] for span in spans], top)
            acc_out[rows, number * DH : (number + 1) * DH] = acc
            stat_out[rows, h : h + 1] = top
            stat_out[rows, hd + h : hd + h + 1] = total
        return carry

    lax.fori_loop(0, lists[row + 3, 0], step, 0)


def near_attend(plan, heads, lists, scal, after, q, ins):
    pool = plan.heads * plan.per_head * B
    return pl.pallas_call(
        functools.partial(near_body, plan, heads),
        out_shape=(
            jax.ShapeDtypeStruct((q.shape[0], len(heads) * DH), jnp.float32),
            jax.ShapeDtypeStruct((q.shape[0], LANES), jnp.float32),
        ),
        in_specs=[SMEM, SMEM, ANY, VMEM] + [HBM] * len(ins),
        out_specs=(VMEM, VMEM),
        scratch_shapes=[
            pltpu.VMEM((pool, DH), jnp.bfloat16),
            pltpu.VMEM((pool, DH), jnp.bfloat16),
            pltpu.SemaphoreType.DMA((8 * plan.heads,)),
        ],
        name="near_attend",
    )(lists, scal, after, q, *ins)


def far_scores_body(plan, sizes, lists, table, after, q, k, low, high, shared, *refs):
    count = PARTS * plan.bits
    chunks, (p_out, stat_out), (near, far, sem) = refs[:count], refs[count : count + 2], refs[count + 2 :]
    hd = plan.heads
    copies = []
    start_far(plan, sizes, chunks, far, sem, copies)
    start_near(plan, range(hd), k, low, high, shared, 0, near, sem, copies)
    for copy in copies:
        copy.wait()
    row = 2 * plan.bits

    def step(kk, carry):
        i = lists[row + 2, kk]
        rows = pl.ds(pl.multiple_of(i * B, B), B)

        def some_heads(g, carry):
            for n in range(UNROLL):
                h = g * UNROLL + n
                qt = q[rows, pl.ds(pl.multiple_of(h * DH, DH), DH)]
                scores = [
                    scores_of(qt, tile_reader(plan, near, far, table[i * R + r, h]))
                    for r in range(R)
                ]
                top = peak(scores)
                total = 0.0
                for r, s in enumerate(scores):
                    p = jnp.exp2((s - top) * FACTOR)
                    total = total + jnp.sum(p, axis=1, keepdims=True)
                    at = pl.multiple_of((h * R + r) * B, B)
                    p_out[rows, pl.ds(at, B)] = p.astype(jnp.bfloat16)
                put_stats(stat_out, rows, hd, h, top, total)
            return carry

        return lax.fori_loop(0, hd // UNROLL, some_heads, carry)

    lax.fori_loop(0, lists[row + 3, 0], step, 0)


def pools_of(plan):
    return [
        pltpu.VMEM((plan.heads * plan.per_head * B, DH), jnp.bfloat16),
        pltpu.VMEM((sum(plan.full), B, DH), jnp.bfloat16),
        pltpu.SemaphoreType.DMA((4 * plan.heads + PARTS * plan.bits,)),
    ]


def far_scores(plan, sizes, lists, table, after, q, k, low, high, shared, chunks):
    return pl.pallas_call(
        functools.partial(far_scores_body, plan, sizes),
        out_shape=(
            jax.ShapeDtypeStruct((q.shape[0], plan.heads * R * B), jnp.bfloat16),
            jax.ShapeDtypeStruct((q.shape[0], LANES), jnp.float32),
        ),
        in_specs=[SMEM, SMEM, ANY, VMEM] + [HBM] * (4 + len(chunks)),
        out_specs=(VMEM, VMEM),
        scratch_shapes=pools_of(plan),
        name="far_scores",
    )(lists, table, after, q, k, low, high, shared, *chunks)


def far_values_body(plan, sizes, heads, lists, table, after, p, pstat, acc_in, stat, v, low, high,
                    shared, *refs):
    count = PARTS * plan.bits
    chunks, out, (near, far, sem) = refs[:count], refs[count], refs[count + 1 :]
    hd = plan.heads
    copies = []
    start_far(plan, sizes, chunks, far, sem, copies)
    start_near(plan, heads, v, low, high, shared, 1, near, sem, copies)
    for copy in copies:
        copy.wait()
    row = 2 * plan.bits

    def step(kk, carry):
        i = lists[row + 2, kk]
        rows = pl.ds(pl.multiple_of(i * B, B), B)
        for number, h in enumerate(heads):
            acc = 0.0
            for r in range(R):
                acc = acc + jnp.dot(
                    p[rows, (number * R + r) * B : (number * R + r + 1) * B],
                    tile_reader(plan, near, far, table[i * R + r, h]),
                    preferred_element_type=jnp.float32,
                )
            far_top, near_top = pstat[rows, h : h + 1], stat[rows, h : h + 1]
            top = jnp.maximum(far_top, near_top)
            a = jnp.exp2((far_top - top) * FACTOR)
            c = jnp.exp2((near_top - top) * FACTOR)
            total = a * pstat[rows, hd + h : hd + h + 1] + c * stat[rows, hd + h : hd + h + 1]
            scale = 1.0 / total
            acc = (a * scale) * acc + (c * scale) * acc_in[rows, number * DH : (number + 1) * DH]
            out[rows, number * DH : (number + 1) * DH] = acc.astype(jnp.bfloat16)
        return carry

    lax.fori_loop(0, lists[row + 3, 0], step, 0)


def far_values(plan, sizes, heads, lists, table, after, p, pstat, acc, stat, v, low, high, shared,
               chunks):
    size = len(heads)
    half = acc.shape[1] // DH
    assert heads[0] % size == 0 and half % size == 0

    def of_team(x, width, first):
        return pl.BlockSpec((x.shape[0], size * width), lambda _: (0, first // size))

    return pl.pallas_call(
        functools.partial(far_values_body, plan, sizes, heads),
        out_shape=jax.ShapeDtypeStruct((p.shape[0], len(heads) * DH), jnp.bfloat16),
        grid=(1,),
        in_specs=[SMEM, SMEM, ANY, of_team(p, R * B, heads[0]), VMEM,
                  of_team(acc, DH, heads[0] % half), VMEM]
        + [HBM] * (4 + len(chunks)),
        out_specs=VMEM,
        scratch_shapes=pools_of(plan),
        name="far_values",
    )(lists, table, after, p, pstat, acc, stat, v, low, high, shared, *chunks)


def body(queries, keys, values, random_holder, random_offset, keep):
    tok_dev, width_dev = queries.shape
    blk_dev = tok_dev // B
    head_dev = width_dev // DH
    count = lax.axis_size("seq")
    groups = lax.axis_size("head")
    plan = Plan(count, groups, blk_dev, head_dev)
    bits = plan.bits
    me = lax.axis_index("seq")
    scal = jnp.stack((me, lax.axis_index("head"))).astype(jnp.int32)

    ids = (random_holder * blk_dev + random_offset).reshape(head_dev, plan.req).T
    asked = jnp.where(jnp.repeat(keep, R)[:, None] > 0, ids, -1)
    mine = jnp.concatenate((asked, jnp.broadcast_to(keep[:, None], (blk_dev, head_dev))), axis=0)
    everyone = lax.all_to_all(
        jnp.broadcast_to(mine[None], (count * groups,) + mine.shape),
        ("seq", "head"), split_axis=0, concat_axis=0, tiled=True,
    )
    everyone = jnp.transpose(everyone, (1, 0, 2)).reshape(mine.shape[0], plan.lanes)
    lists, table = make_lists(plan, scal, everyone, ids)

    blk_bits = log2(blk_dev)
    rows = B // PARTS
    row = 2 * bits
    cuts = [0] + [cut for cut in SPLIT if cut < head_dev] + [head_dev]
    teams = [range(low, high) for low, high in zip(cuts, cuts[1:])]
    flags = lambda cond: jnp.concatenate((scal, cond.astype(jnp.int32)[None]))
    odd = flags((me & 1) == 1)

    def branch(sizes, csizes):
        def steps(queries, keys, values, lists, table, scal, odd):
            got = [[] for _ in range(2 * PARTS)]
            last = [lists]

            def run_after(fn, *args):
                out = fn(last[0], *args)
                last[0] = out[0] if isinstance(out, (tuple, list)) else out
                return out

            def hop(x, pairs):
                return lax.ppermute(x, "seq", pairs)

            def swap(x, bit, count, down_only=False):
                return hop(x, [(i, i ^ bit) for i in range(count) if not down_only or i & bit])

            def packed_tiles(s, chunk):
                which, part = chunk // PARTS, chunk % PARTS
                bases = [plan.own + at for at in plan.base[: s + 1]]
                return run_after(
                    lambda after: pack(
                        s, sizes[s], bases, tile_part(blk_bits, part, rows), rows, lists, after,
                        [(keys, values)[which]] + got[chunk], DH,
                    )
                )

            def stage(s, chunk):
                got[chunk].append(swap(packed_tiles(s, chunk), count >> (s + 1), count))

            def tiles(which):
                return [
                    x.reshape(-1, rows, DH)
                    for part in range(PARTS)
                    for x in got[which * PARTS + part]
                ]

            def begin(chunk, packed):
                packed = run_after(lambda after: hold(after, got[chunk - 1][0], packed))
                got[chunk].append(swap(packed, count >> 1, count))

            stage(0, 0)
            low, high, first_keys, first_values = run_after(edges, keys, values)
            low = hop(low, [(i, i + 1) for i in range(count - 1)])
            high = hop(high, [(i + 1, i) for i in range(count - 1)])
            beside = hop(first_values, [(0, 1)])
            coming = packed_tiles(0, 1)
            held = run_after(either, odd, first_keys, beside)
            spreads = []
            for s in range(bits - 1):
                bit = count >> (s + 1)
                spreads.append(
                    (bit, [(i + j, i + j + bit) for i in range(0, count, 2 * bit) for j in (0, 1)])
                )
            chunks = 2 * PARTS
            last_spread = max(len(spreads), chunks - 2)
            nears = []

            def near_half(number):
                half = head_dev // 2
                return run_after(
                    lambda after: near_attend(
                        plan, range(number * half, (number + 1) * half), lists, scal, after,
                        queries, [keys, values, low, high, shared_keys, shared_values],
                    )
                )

            for step in range(chunks + bits - 1):
                there = None
                if step < len(spreads):
                    bit, pairs = spreads[step]
                    there = hop(held, pairs)
                elif step == len(spreads):
                    there = swap(held, 1, count)
                if step + 1 < chunks:
                    begin(step + 1, coming)
                for s in range(1, bits):
                    if s == 2 and step == max(chunks - 1, len(spreads) + 1):
                        nears.append(near_half(1))
                    if 0 <= step + 1 - s < chunks:
                        stage(s, step + 1 - s)
                    if s == 1 and step + 2 < chunks:
                        coming = packed_tiles(0, step + 2)
                if step < len(spreads):
                    held = run_after(either, flags((me & bit) != 0), held, there)
                elif step == len(spreads):
                    shared_keys = run_after(either, odd, held, there)
                    shared_values = run_after(either, odd, there, held)
                if step == 1:
                    low = run_after(hold, high, low)
                if step == last_spread:
                    nears.append(near_half(0))
                if step == max(chunks, last_spread):
                    p, pstat = run_after(
                        lambda after: far_scores(
                            plan, sizes, lists, table, after, queries, keys, low, high,
                            shared_keys, tiles(0),
                        )
                    )
            if len(nears) == 1:
                nears.append(near_half(1))

            sources = []

            def pack_stage(s, held):
                bases = [plan.blk + at for at in plan.cbase[: s + 1]]
                packed = run_after(
                    lambda after: pack(
                        bits + s, csizes[s], bases, block_part, B, lists, after, held,
                        held[0].shape[1],
                    )
                )
                held.append(swap(packed, count >> (s + 1), count, s == 0))

            for half, heads in enumerate(teams):
                acc, stat = nears[heads[0] // (head_dev // 2)]
                attended = run_after(
                    lambda after: far_values(
                        plan, sizes, heads, lists, table, after, p, pstat, acc, stat, values,
                        low, high, shared_values, tiles(1),
                    )
                )
                sources.append([attended])
                pack_stage(0, sources[half])
            for step in range(len(teams) + bits - 2):
                for s in range(1, bits):
                    if 0 <= step + 1 - s < len(teams):
                        pack_stage(s, sources[step + 1 - s])
            bases = [plan.blk + at for at in plan.cbase + [sum(plan.cfull)]]
            widths = [len(heads) * DH for heads in teams]
            return final(row, blk_dev, bases, lists, sum(sources, []), widths)

        return steps

    return lax.switch(
        lists[row + 1, 0],
        [branch(a, c) for a, c in zip(plan.route_sizes(), plan.pack_sizes())],
        queries, keys, values, lists, table, scal, odd,
    )


def solution(mesh):
    in_specs = (
        P("seq", "head"),
        P("seq", "head"),
        P("seq", "head"),
        P("head", "seq", None),
        P("head", "seq", None),
        P("seq"),
    )
    out_specs = P("seq", "head")
    return jax.shard_map(body, mesh=mesh, in_specs=in_specs, out_specs=out_specs, check_vma=False)
```

```python
import functools
import math

import jax
import jax.numpy as jnp
from jax import lax
from jax.experimental import pallas as pl
from jax.experimental.pallas import tpu as pltpu
from jax.sharding import PartitionSpec as P


DH = 128
B = 128
G = 2
R = 3
LANES = 128

neg_big = -1e30

ROUTE_SHARES = ((0.65, 0.56, 0.645), (0.71, 0.6, 0.705), (1.0, 1.0, 1.0))
PACK_SHARES = ((0.7, 0.35, 0.75), (0.85, 0.42, 0.75), (1.0, 1.0, 1.0))
CHUNKS = ((0, 0, 64), (0, 64, 64), (1, 0, 48), (1, 48, 48), (1, 96, 32))
UNROLL = 4
PAIR = 2
SPLIT = (2, 4, 6)


def log2(size):
    assert size & (size - 1) == 0
    return size.bit_length() - 1


class Plan:
    def __init__(self, count, groups, blk_dev, head_dev):
        self.count, self.groups, self.blk, self.heads = count, groups, blk_dev, head_dev
        self.bits = log2(count)
        self.stride = groups * head_dev
        self.lanes = count * self.stride
        self.blocks = count * blk_dev
        self.req = blk_dev * R
        self.per_head = blk_dev + 2 + G
        self.own = blk_dev * head_dev
        most = max(2, (self.req + count - 1) // count)
        bound = (count // 2) * most * head_dev
        self.full = [min(self.own << s, bound) for s in range(self.bits)]
        self.base = [sum(self.full[:s]) for s in range(self.bits)]
        self.cfull = [
            min((blk_dev - 1) << s, blk_dev << (self.bits - 1 - s)) for s in range(self.bits)
        ]
        self.cbase = [sum(self.cfull[:s]) for s in range(self.bits)]
        self.width = -(-max(self.full + self.cfull) // LANES) * LANES

    def sizes(self, full, shares):
        out = []
        for s in range(self.bits):
            share = shares[0] if s == 0 else shares[2] if s == self.bits - 1 else shares[1]
            out.append(min(full[s], max(1, math.ceil(full[s] * share))))
        return out

    def route_sizes(self):
        return [self.sizes(self.full, shares) for shares in ROUTE_SHARES]

    def pack_sizes(self):
        return [self.sizes(self.cfull, shares) for shares in PACK_SHARES]

    def rows(self):
        return 2 * self.bits + 4


def iota(shape, axis):
    return lax.broadcasted_iota(jnp.int32, shape, axis)


def flag(cond):
    return jnp.where(cond, 1.0, 0.0)


def dot(a, b):
    return jnp.dot(
        a.astype(jnp.bfloat16), b.astype(jnp.bfloat16), preferred_element_type=jnp.float32
    )


def choose(tops, sizes):
    index = jnp.int32(len(sizes) - 1)
    for number in reversed(range(len(sizes) - 1)):
        fits = functools.reduce(
            jnp.logical_and, [top <= float(size) for top, size in zip(tops, sizes[number])]
        )
        index = jnp.where(fits, jnp.int32(number), index)
    return index


def lists_body(plan, scal, ids, own_ids, lists, table):
    me, group = scal[0], scal[1]
    T, L, hd = plan.blocks, plan.lanes, plan.heads
    lb, ls, lh = log2(plan.blk), log2(plan.stride), log2(hd)
    W = plan.width
    t = iota((T, L), 0)
    lane = iota((T, L), 1)
    holder = jnp.right_shift(lane, ls)
    need = jnp.zeros((T, L), jnp.int32)
    for k in range(plan.req):
        need = jnp.where(t == ids[k : k + 1, :], 1, need)
    near = (t >= holder * plan.blk - 1) & (t <= (holder + 1) * plan.blk)
    need = jnp.where(near | (t < G), 0, need)
    needb = need.astype(jnp.float32).astype(jnp.bfloat16)
    x = iota((L, L), 0)
    y = iota((L, L), 1)
    lower = flag(iota((T, T), 0) > iota((T, T), 1)).astype(jnp.bfloat16)
    upper = flag(iota((hd, hd), 0) < iota((hd, hd), 1)).astype(jnp.bfloat16)
    same = flag(jnp.right_shift(x, lh) == jnp.right_shift(y, lh)).astype(jnp.bfloat16)
    xe = iota((L, hd), 0)
    he = iota((L, hd), 1)
    th = iota((T, hd), 0)
    hh = iota((T, hd), 1)
    blk_of = jnp.right_shift(th, lb)
    pos_of = th & (plan.blk - 1)
    is_own = blk_of == me
    loc = jnp.where(is_own, jnp.left_shift(hh, lb) + pos_of, 0)
    slot_w = iota((T, W), 1)
    tops = []

    def order(mask):
        within = jnp.dot(lower, mask.astype(jnp.bfloat16), preferred_element_type=jnp.float32)
        cols = jnp.broadcast_to(jnp.sum(mask, axis=0, keepdims=True), (8, hd))
        return within + dot(cols, upper)[0:1, :]

    for s in range(plan.bits):
        b = plan.bits - 1 - s
        free = ((1 << b) - 1) << ls
        group_of = flag(((x ^ y) & ~free) == 0).astype(jnp.bfloat16)
        wanted = jnp.dot(needb, group_of, preferred_element_type=jnp.float32)
        into = ((jnp.right_shift(t, lb) ^ holder ^ (1 << b)) & ((2 << b) - 1)) == 0
        recv = flag((wanted > 0.5) & into)
        cols = jnp.broadcast_to(jnp.sum(recv, axis=0, keepdims=True), (8, L))
        tops.append(jnp.max(dot(cols, same)))
        recvb = recv.astype(jnp.bfloat16)
        mine = flag(xe == me * plan.stride + group * hd + he).astype(jnp.bfloat16)
        theirs = flag(xe == (me ^ (1 << b)) * plan.stride + group * hd + he).astype(jnp.bfloat16)
        got = jnp.dot(recvb, mine, preferred_element_type=jnp.float32)
        sent = jnp.dot(recvb, theirs, preferred_element_type=jnp.float32)
        place = jnp.where(sent > 0.5, order(sent).astype(jnp.int32), -1)
        line = jnp.zeros((1, W), jnp.int32)
        for h in range(hd):
            hit = place[:, h : h + 1] == slot_w
            line = line + jnp.sum(
                jnp.where(hit, loc[:, h : h + 1] + 1, 0), axis=0, keepdims=True
            )
        lists[s : s + 1, :] = line
        loc = jnp.where(
            got > 0.5, plan.own + plan.base[s] + order(got).astype(jnp.int32), loc
        )
    per = plan.per_head
    at = jnp.where(is_own, hh * per + 1 + pos_of, loc + hd * (per - plan.blk))
    at = jnp.where(th == me * plan.blk - 1, hh * per, at)
    at = jnp.where(th == (me + 1) * plan.blk, hh * per + 1 + plan.blk, at)
    at = jnp.where((th < G) & ~is_own, hh * per + 2 + plan.blk + th, at)
    for k in range(plan.req):
        hit = th == own_ids[k : k + 1, :]
        table[k : k + 1, 0:hd] = jnp.sum(jnp.where(hit, at, 0), axis=0, keepdims=True)

    kept = jnp.zeros((T, L), jnp.int32)
    head_lane = (jnp.right_shift(t, lb) == holder) & ((lane & (plan.stride - 1)) == 0)
    for i in range(plan.blk):
        hit = head_lane & ((t & (plan.blk - 1)) == i)
        kept = kept + jnp.where(hit, ids[plan.req + i : plan.req + i + 1, :], 0)
    kept = jnp.broadcast_to(jnp.sum(kept, axis=1, keepdims=True), (T, W))
    tw = iota((T, W), 0)
    dev = jnp.right_shift(tw, lb)

    def before(mask):
        return jnp.dot(
            lower, mask.astype(jnp.float32).astype(jnp.bfloat16), preferred_element_type=jnp.float32
        ).astype(jnp.int32)

    rank = before(kept)
    dest = jnp.right_shift(rank, lb)
    cloc = jnp.where(dev == me, tw & (plan.blk - 1), 0)
    ctops = []
    for s in range(plan.bits):
        b = plan.bits - 1 - s
        ok = (kept > 0) & (jnp.right_shift(dest ^ slot_w, b) == 0)
        ok = ok & (((dev ^ slot_w ^ (1 << b)) & ((2 << b) - 1)) == 0)
        recv = jnp.where(ok, 1, 0)
        ctops.append(jnp.max(jnp.sum(recv.astype(jnp.float32), axis=0, keepdims=True)))
        got = jnp.sum(jnp.where(slot_w == me, recv, 0), axis=1, keepdims=True)
        sent = jnp.sum(jnp.where(slot_w == (me ^ (1 << b)), recv, 0), axis=1, keepdims=True)
        got = jnp.broadcast_to(got, (T, W))
        sent = jnp.broadcast_to(sent, (T, W))
        hit = (sent > 0) & (before(sent) == slot_w)
        row = plan.bits + s
        lists[row : row + 1, :] = jnp.sum(jnp.where(hit, cloc + 1, 0), axis=0, keepdims=True)
        cloc = jnp.where(got > 0, plan.blk + plan.cbase[s] + before(got), cloc)
    row = 2 * plan.bits
    hit = (kept > 0) & (rank == me * plan.blk + slot_w) & (slot_w < plan.blk)
    lists[row : row + 1, :] = jnp.sum(jnp.where(hit, cloc + 1, 0), axis=0, keepdims=True)
    both = [a + c for a, c in zip(plan.route_sizes(), plan.pack_sizes())]
    lists[row + 1 : row + 2, :] = jnp.broadcast_to(choose(tops + ctops, both), (1, W))
    first = jnp.sum(jnp.where(tw < me * plan.blk, kept, 0), axis=0, keepdims=True)
    hit = (kept > 0) & (dev == me) & (rank - first == slot_w)
    lists[row + 2 : row + 3, :] = jnp.sum(
        jnp.where(hit, tw & (plan.blk - 1), 0), axis=0, keepdims=True
    )
    lists[row + 3 : row + 4, :] = jnp.sum(
        jnp.where((dev == me), kept, 0), axis=0, keepdims=True
    )


SMEM = pl.BlockSpec(memory_space=pltpu.SMEM)
VMEM = pl.BlockSpec(memory_space=pltpu.VMEM)
HBM = pl.BlockSpec(memory_space=pltpu.HBM)
ANY = pl.BlockSpec(memory_space=pl.ANY)


def make_lists(plan, scal, ids, own_ids):
    return pl.pallas_call(
        functools.partial(lists_body, plan),
        out_shape=(
            jax.ShapeDtypeStruct((plan.rows(), plan.width), jnp.int32),
            jax.ShapeDtypeStruct((plan.req, LANES), jnp.int32),
        ),
        in_specs=[SMEM, VMEM, VMEM],
        out_specs=(VMEM, VMEM),
        name="make_lists",
    )(scal, ids, own_ids)


def pack_body(row, size, bases, own_part, rows, lists, *refs):
    sources, out = refs[1:-1], refs[-1]

    def step(j, carry):
        code = jnp.maximum(lists[row, j] - 1, 0)
        target = pl.ds(pl.multiple_of(j * rows, rows), rows)

        @pl.when(code < bases[0])
        def _():
            out[target, :] = own_part(sources[0], code)

        for number, source in enumerate(sources[1:]):
            low = bases[number]

            @pl.when((code >= low) & (code < bases[number + 1]))
            def _():
                at = pl.multiple_of((code - low) * rows, rows)
                out[target, :] = source[pl.ds(at, rows), :]

        return carry

    lax.fori_loop(0, size, step, 0)


def pack(row, size, bases, own_part, rows, lists, after, sources, width):
    return pl.pallas_call(
        functools.partial(pack_body, row, size, bases, own_part, rows),
        out_shape=jax.ShapeDtypeStruct((size * rows, width), jnp.bfloat16),
        in_specs=[SMEM, ANY] + [VMEM] * len(sources),
        out_specs=VMEM,
    )(lists, after, *sources)


def either_body(after, scal, a, b, out):
    @pl.when(scal[2] == 0)
    def _():
        out[...] = a[...]

    @pl.when(scal[2] != 0)
    def _():
        out[...] = b[...]


def either(after, cond, a, b):
    return pl.pallas_call(
        either_body,
        out_shape=jax.ShapeDtypeStruct(a.shape, a.dtype),
        in_specs=[ANY, SMEM, VMEM, VMEM],
        out_specs=VMEM,
        name="either",
    )(after, cond, a, b)


def edges_body(after, keys, values, low, high, first_keys, first_values):
    tokens, width = keys.shape
    low[:, :width] = keys[tokens - B : tokens, :]
    low[:, width:] = values[tokens - B : tokens, :]
    high[:, :width] = keys[:B, :]
    high[:, width:] = values[:B, :]
    first_keys[...] = keys[: G * B, :]
    first_values[...] = values[: G * B, :]


def edges(after, keys, values):
    width, dtype = keys.shape[1], keys.dtype
    block = jax.ShapeDtypeStruct((B, 2 * width), dtype)
    shared = jax.ShapeDtypeStruct((G * B, width), dtype)
    return pl.pallas_call(
        edges_body,
        out_shape=(block, block, shared, shared),
        in_specs=[ANY, VMEM, VMEM],
        out_specs=(VMEM,) * 4,
        name="edges",
    )(after, keys, values)


def hold_body(after, before, x, out):
    pass


def hold(after, before, x):
    return pl.pallas_call(
        hold_body,
        out_shape=jax.ShapeDtypeStruct(x.shape, x.dtype),
        in_specs=[ANY, ANY, ANY],
        out_specs=ANY,
        input_output_aliases={2: 0},
        name="hold",
    )(after, before, x)


def tile_part(heads_bits, first, rows):
    def read(own, code):
        head = jnp.right_shift(code, heads_bits)
        pos = code & ((1 << heads_bits) - 1)
        at = pl.multiple_of(pos * B + first, 16)
        return own[pl.ds(at, rows), pl.ds(pl.multiple_of(head * DH, DH), DH)]

    return read


def block_part(own, code):
    return own[pl.ds(pl.multiple_of(code * B, B), B), :]


def final_body(row, slots, bases, widths, lists, *refs):
    out = refs[-1]
    per = (len(refs) - 1) // len(widths)

    def step(j, carry):
        code = lists[row, j]
        target = pl.ds(pl.multiple_of(j * B, B), B)

        @pl.when(code == 0)
        def _():
            out[target, :] = jnp.zeros((B, out.shape[1]), out.dtype)

        for number in range(per):
            low = 0 if number == 0 else bases[number - 1]

            @pl.when((code - 1 >= low) & (code - 1 < bases[number]))
            def _():
                at = pl.multiple_of((code - 1 - low) * B, B)
                for part, width in enumerate(widths):
                    first = sum(widths[:part])
                    out[target, first : first + width] = refs[part * per + number][
                        pl.ds(at, B), :
                    ]

        return carry

    lax.fori_loop(0, slots, step, 0)


def final(row, slots, bases, lists, sources, widths):
    return pl.pallas_call(
        functools.partial(final_body, row, slots, bases, widths),
        out_shape=jax.ShapeDtypeStruct((slots * B, sum(widths)), jnp.bfloat16),
        in_specs=[SMEM] + [VMEM] * len(sources),
        out_specs=VMEM,
        name="place_blocks",
    )(lists, *sources)


FACTOR = math.log2(math.e) / math.sqrt(DH)


def scores_of(qt, kt):
    return lax.dot_general(
        qt, kt, (((1,), (1,)), ((), ())), preferred_element_type=jnp.float32
    )


def gather_parts(scores, values, top):
    total = 0.0
    acc = 0.0
    for s, vt in zip(scores, values):
        p = jnp.exp2((s - top) * FACTOR)
        total = total + jnp.sum(p, axis=1, keepdims=True)
        acc = acc + jnp.dot(p.astype(jnp.bfloat16), vt, preferred_element_type=jnp.float32)
    return total, acc


def peak(scores):
    return functools.reduce(jnp.maximum, [jnp.max(s, axis=1, keepdims=True) for s in scores])


def start_near(plan, heads, own, low, high, shared, first, pool, sem, copies):
    wide = plan.heads * DH
    for h in heads:
        cols = pl.ds(h * DH, DH)
        there = pl.ds(first * wide + h * DH, DH)
        for source, at, tiles in (
            (low.at[:, there], 0, 1),
            (own.at[:, cols], 1, plan.blk),
            (high.at[:, there], 1 + plan.blk, 1),
            (shared.at[:, cols], 2 + plan.blk, G),
        ):
            copy = pltpu.make_async_copy(
                source,
                pool.at[pl.ds((h * plan.per_head + at) * B, tiles * B), :],
                sem.at[len(copies)],
            )
            copy.start()
            copies.append(copy)


def parts_of(which):
    return [(first, rows) for kind, first, rows in CHUNKS if kind == which]


def start_far(plan, sizes, which, chunks, pool, sem, copies):
    for part, (first, rows) in enumerate(parts_of(which)):
        for s in range(plan.bits):
            copy = pltpu.make_async_copy(
                chunks[part * plan.bits + s],
                pool.at[pl.ds(plan.base[s], sizes[s]), pl.ds(first, rows), :],
                sem.at[len(copies)],
            )
            copy.start()
            copies.append(copy)


def tile_reader(plan, near_pool, far_pool, at):
    split = plan.heads * plan.per_head
    inside = at < split
    row = pl.multiple_of(jnp.where(inside, at, 0) * B, B)
    near = near_pool[pl.ds(row, B), :]
    far = far_pool[jnp.where(inside, 0, at - split)]
    return jnp.where(inside, near, far)


def put_stats(stat, rows, hd, h, top, total):
    lane = lax.broadcasted_iota(jnp.int32, (B, LANES), 1)
    old = stat[rows, :]
    stat[rows, :] = jnp.where(lane == h, top, jnp.where(lane == hd + h, total, old))


def near_body(plan, heads, lists, scal, after, q, *refs):
    k, v, low, high, shared_k, shared_v, acc_out, stat_out, kp, vp, sem = refs
    blk, hd, per = plan.blk, plan.heads, plan.per_head
    copies = []
    start_near(plan, heads, k, low, high, shared_k, 0, kp, sem, copies)
    start_near(plan, heads, v, low, high, shared_v, 1, vp, sem, copies)
    for copy in copies:
        copy.wait()
    me = scal[0]
    row = 2 * plan.bits
    win = 3 * B

    def step(kk, carry):
        i = lists[row + 2, kk]
        first = (me * blk + i) == 0
        last = (me * blk + i) == plan.blocks - 1
        col = lax.broadcasted_iota(jnp.int32, (B, win), 1)
        dead = (first & (col < B)) | (last & (col >= 2 * B))
        rows = pl.ds(pl.multiple_of(i * B, B), B)

        def some_heads(g, carry):
            for n in range(PAIR):
                number = g * PAIR + n
                h = heads[0] + number
                qt = q[rows, pl.ds(pl.multiple_of(h * DH, DH), DH)]
                spans = (
                    pl.ds(pl.multiple_of((h * per + i) * B, B), win),
                    pl.ds(pl.multiple_of((h * per + 2 + blk) * B, B), G * B),
                )
                scores = [scores_of(qt, kp[span, :]) for span in spans]
                scores[0] = jnp.where(dead, neg_big, scores[0])
                top = peak(scores)
                total, acc = gather_parts(scores, [vp[span, :] for span in spans], top)
                acc_out[rows, pl.ds(pl.multiple_of(number * DH, DH), DH)] = acc
                put_stats(stat_out, rows, hd, h, top, total)
            return carry

        return lax.fori_loop(0, len(heads) // PAIR, some_heads, carry)

    lax.fori_loop(0, lists[row + 3, 0], step, 0)


def near_attend(plan, heads, lists, scal, after, q, ins):
    pool = plan.heads * plan.per_head * B
    return pl.pallas_call(
        functools.partial(near_body, plan, heads),
        out_shape=(
            jax.ShapeDtypeStruct((q.shape[0], len(heads) * DH), jnp.float32),
            jax.ShapeDtypeStruct((q.shape[0], LANES), jnp.float32),
        ),
        in_specs=[SMEM, SMEM, ANY, VMEM] + [HBM] * len(ins),
        out_specs=(VMEM, VMEM),
        scratch_shapes=[
            pltpu.VMEM((pool, DH), jnp.bfloat16),
            pltpu.VMEM((pool, DH), jnp.bfloat16),
            pltpu.SemaphoreType.DMA((8 * plan.heads,)),
        ],
        name="near_attend",
    )(lists, scal, after, q, *ins)


def far_scores_body(plan, sizes, lists, table, after, q, k, low, high, shared, *refs):
    count = len(parts_of(0)) * plan.bits
    chunks, (p_out, stat_out), (near, far, sem) = refs[:count], refs[count : count + 2], refs[count + 2 :]
    hd = plan.heads
    copies = []
    start_far(plan, sizes, 0, chunks, far, sem, copies)
    start_near(plan, range(hd), k, low, high, shared, 0, near, sem, copies)
    for copy in copies:
        copy.wait()
    row = 2 * plan.bits

    def step(kk, carry):
        i = lists[row + 2, kk]
        rows = pl.ds(pl.multiple_of(i * B, B), B)

        def some_heads(g, carry):
            for n in range(UNROLL):
                h = g * UNROLL + n
                qt = q[rows, pl.ds(pl.multiple_of(h * DH, DH), DH)]
                scores = [
                    scores_of(qt, tile_reader(plan, near, far, table[i * R + r, h]))
                    for r in range(R)
                ]
                top = peak(scores)
                total = 0.0
                for r, s in enumerate(scores):
                    p = jnp.exp2((s - top) * FACTOR)
                    total = total + jnp.sum(p, axis=1, keepdims=True)
                    at = pl.multiple_of((h * R + r) * B, B)
                    p_out[rows, pl.ds(at, B)] = p.astype(jnp.bfloat16)
                put_stats(stat_out, rows, hd, h, top, total)
            return carry

        return lax.fori_loop(0, hd // UNROLL, some_heads, carry)

    lax.fori_loop(0, lists[row + 3, 0], step, 0)


def pools_of(plan):
    return [
        pltpu.VMEM((plan.heads * plan.per_head * B, DH), jnp.bfloat16),
        pltpu.VMEM((sum(plan.full), B, DH), jnp.bfloat16),
        pltpu.SemaphoreType.DMA((4 * plan.heads + len(CHUNKS) * plan.bits,)),
    ]


def far_scores(plan, sizes, lists, table, after, q, k, low, high, shared, chunks):
    return pl.pallas_call(
        functools.partial(far_scores_body, plan, sizes),
        out_shape=(
            jax.ShapeDtypeStruct((q.shape[0], plan.heads * R * B), jnp.bfloat16),
            jax.ShapeDtypeStruct((q.shape[0], LANES), jnp.float32),
        ),
        in_specs=[SMEM, SMEM, ANY, VMEM] + [HBM] * (4 + len(chunks)),
        out_specs=(VMEM, VMEM),
        scratch_shapes=pools_of(plan),
        name="far_scores",
    )(lists, table, after, q, k, low, high, shared, *chunks)


def far_values_body(plan, sizes, heads, lists, table, after, p, pstat, acc_in, stat, v, low, high,
                    shared, *refs):
    count = len(parts_of(1)) * plan.bits
    chunks, out, (near, far, sem) = refs[:count], refs[count], refs[count + 1 :]
    hd = plan.heads
    copies = []
    start_far(plan, sizes, 1, chunks, far, sem, copies)
    start_near(plan, heads, v, low, high, shared, 1, near, sem, copies)
    for copy in copies:
        copy.wait()
    row = 2 * plan.bits

    def step(kk, carry):
        i = lists[row + 2, kk]
        rows = pl.ds(pl.multiple_of(i * B, B), B)
        for number, h in enumerate(heads):
            acc = 0.0
            for r in range(R):
                acc = acc + jnp.dot(
                    p[rows, (number * R + r) * B : (number * R + r + 1) * B],
                    tile_reader(plan, near, far, table[i * R + r, h]),
                    preferred_element_type=jnp.float32,
                )
            far_top, near_top = pstat[rows, h : h + 1], stat[rows, h : h + 1]
            top = jnp.maximum(far_top, near_top)
            a = jnp.exp2((far_top - top) * FACTOR)
            c = jnp.exp2((near_top - top) * FACTOR)
            total = a * pstat[rows, hd + h : hd + h + 1] + c * stat[rows, hd + h : hd + h + 1]
            scale = 1.0 / total
            acc = (a * scale) * acc + (c * scale) * acc_in[rows, number * DH : (number + 1) * DH]
            out[rows, number * DH : (number + 1) * DH] = acc.astype(jnp.bfloat16)
        return carry

    lax.fori_loop(0, lists[row + 3, 0], step, 0)


def far_values(plan, sizes, heads, lists, table, after, p, pstat, acc, stat, v, low, high, shared,
               chunks):
    size = len(heads)
    half = acc.shape[1] // DH
    assert heads[0] % size == 0 and half % size == 0

    def of_team(x, width, first):
        return pl.BlockSpec((x.shape[0], size * width), lambda _: (0, first // size))

    return pl.pallas_call(
        functools.partial(far_values_body, plan, sizes, heads),
        out_shape=jax.ShapeDtypeStruct((p.shape[0], len(heads) * DH), jnp.bfloat16),
        grid=(1,),
        in_specs=[SMEM, SMEM, ANY, of_team(p, R * B, heads[0]), VMEM,
                  of_team(acc, DH, heads[0] % half), VMEM]
        + [HBM] * (4 + len(chunks)),
        out_specs=VMEM,
        scratch_shapes=pools_of(plan),
        name="far_values",
    )(lists, table, after, p, pstat, acc, stat, v, low, high, shared, *chunks)


def body(queries, keys, values, random_holder, random_offset, keep):
    tok_dev, width_dev = queries.shape
    blk_dev = tok_dev // B
    head_dev = width_dev // DH
    count = lax.axis_size("seq")
    groups = lax.axis_size("head")
    plan = Plan(count, groups, blk_dev, head_dev)
    bits = plan.bits
    me = lax.axis_index("seq")
    scal = jnp.stack((me, lax.axis_index("head"))).astype(jnp.int32)

    ids = (random_holder * blk_dev + random_offset).reshape(head_dev, plan.req).T
    asked = jnp.where(jnp.repeat(keep, R)[:, None] > 0, ids, -1)
    mine = jnp.concatenate((asked, jnp.broadcast_to(keep[:, None], (blk_dev, head_dev))), axis=0)
    everyone = lax.all_to_all(
        jnp.broadcast_to(mine[None], (count * groups,) + mine.shape),
        ("seq", "head"), split_axis=0, concat_axis=0, tiled=True,
    )
    everyone = jnp.transpose(everyone, (1, 0, 2)).reshape(mine.shape[0], plan.lanes)
    lists, table = make_lists(plan, scal, everyone, ids)

    blk_bits = log2(blk_dev)
    row = 2 * bits
    cuts = [0] + [cut for cut in SPLIT if cut < head_dev] + [head_dev]
    teams = [range(low, high) for low, high in zip(cuts, cuts[1:])]
    flags = lambda cond: jnp.concatenate((scal, cond.astype(jnp.int32)[None]))
    odd = flags((me & 1) == 1)

    def branch(sizes, csizes):
        def steps(queries, keys, values, lists, table, scal, odd):
            got = [[] for _ in CHUNKS]
            last = [lists]

            def run_after(fn, *args):
                out = fn(last[0], *args)
                last[0] = out[0] if isinstance(out, (tuple, list)) else out
                return out

            def hop(x, pairs):
                return lax.ppermute(x, "seq", pairs)

            def swap(x, bit, count, down_only=False):
                return hop(x, [(i, i ^ bit) for i in range(count) if not down_only or i & bit])

            def packed_tiles(s, chunk):
                which, first, rows = CHUNKS[chunk]
                bases = [plan.own + at for at in plan.base[: s + 1]]
                return run_after(
                    lambda after: pack(
                        s, sizes[s], bases, tile_part(blk_bits, first, rows), rows, lists, after,
                        [(keys, values)[which]] + got[chunk], DH,
                    )
                )

            def stage(s, chunk):
                got[chunk].append(swap(packed_tiles(s, chunk), count >> (s + 1), count))

            def tiles(which):
                return [
                    x.reshape(-1, rows, DH)
                    for (kind, first, rows), stages in zip(CHUNKS, got)
                    if kind == which
                    for x in stages
                ]

            def begin(chunk, packed):
                packed = run_after(lambda after: hold(after, got[chunk - 1][0], packed))
                got[chunk].append(swap(packed, count >> 1, count))

            stage(0, 0)
            low, high, first_keys, first_values = run_after(edges, keys, values)
            low = hop(low, [(i, i + 1) for i in range(count - 1)])
            high = hop(high, [(i + 1, i) for i in range(count - 1)])
            beside = hop(first_values, [(0, 1)])
            coming = packed_tiles(0, 1)
            held = run_after(either, odd, first_keys, beside)
            spreads = []
            for s in range(bits - 1):
                bit = count >> (s + 1)
                spreads.append(
                    (bit, [(i + j, i + j + bit) for i in range(0, count, 2 * bit) for j in (0, 1)])
                )
            chunks = len(CHUNKS)
            nears = []

            def near_half(number):
                half = head_dev // 2
                return run_after(
                    lambda after: near_attend(
                        plan, range(number * half, (number + 1) * half), lists, scal, after,
                        queries, [keys, values, low, high, shared_keys, shared_values],
                    )
                )

            for step in range(max(chunks + bits - 1, len(spreads) + 2)):
                there = None
                if step < len(spreads):
                    bit, pairs = spreads[step]
                    there = hop(held, pairs)
                elif step == len(spreads):
                    there = swap(held, 1, count)
                if step + 1 < chunks:
                    begin(step + 1, coming)
                for s in range(1, bits):
                    if 0 <= step + 1 - s < chunks:
                        stage(s, step + 1 - s)
                    if s == 1 and step + 2 < chunks:
                        coming = packed_tiles(0, step + 2)
                if step < len(spreads):
                    held = run_after(either, flags((me & bit) != 0), held, there)
                elif step == len(spreads):
                    shared_keys = run_after(either, odd, held, there)
                    shared_values = run_after(either, odd, there, held)
                if step == 1:
                    low = run_after(hold, high, low)
                if step in (len(spreads), len(spreads) + 1):
                    nears.append(near_half(step - len(spreads)))
            p, pstat = run_after(
                lambda after: far_scores(
                    plan, sizes, lists, table, after, queries, keys, low, high, shared_keys,
                    tiles(0),
                )
            )

            sources = []

            def pack_stage(s, held):
                bases = [plan.blk + at for at in plan.cbase[: s + 1]]
                packed = run_after(
                    lambda after: pack(
                        bits + s, csizes[s], bases, block_part, B, lists, after, held,
                        held[0].shape[1],
                    )
                )
                held.append(swap(packed, count >> (s + 1), count, s == 0))

            for step in range(len(teams) + 2 * (bits - 1)):
                if step < len(teams):
                    heads = teams[step]
                    acc, stat = nears[heads[0] // (head_dev // 2)]
                    attended = run_after(
                        lambda after: far_values(
                            plan, sizes, heads, lists, table, after, p, pstat, acc, stat, values,
                            low, high, shared_values, tiles(1),
                        )
                    )
                    sources.append([attended])
                    pack_stage(0, sources[step])
                for s in reversed(range(1, bits)):
                    if 0 <= step - 2 * s < len(teams):
                        pack_stage(s, sources[step - 2 * s])
            bases = [plan.blk + at for at in plan.cbase + [sum(plan.cfull)]]
            widths = [len(heads) * DH for heads in teams]
            return final(row, blk_dev, bases, lists, sum(sources, []), widths)

        return steps

    return lax.switch(
        lists[row + 1, 0],
        [branch(a, c) for a, c in zip(plan.route_sizes(), plan.pack_sizes())],
        queries, keys, values, lists, table, scal, odd,
    )


def solution(mesh):
    in_specs = (
        P("seq", "head"),
        P("seq", "head"),
        P("seq", "head"),
        P("head", "seq", None),
        P("head", "seq", None),
        P("seq"),
    )
    out_specs = P("seq", "head")
    return jax.shard_map(body, mesh=mesh, in_specs=in_specs, out_specs=out_specs, check_vma=False)
```

```python
import functools
import math

import jax
import jax.numpy as jnp
from jax import lax
from jax.experimental import pallas as pl
from jax.experimental.pallas import tpu as pltpu
from jax.sharding import PartitionSpec as P


DH = 128
B = 128
G = 2
R = 3
LANES = 128

neg_big = -1e30

ROUTE_SHARES = ((0.65, 0.555, 0.62), (0.71, 0.6, 0.705), (1.0, 1.0, 1.0))
PACK_SHARES = ((0.7, 0.35, 0.75), (0.85, 0.42, 0.75), (1.0, 1.0, 1.0))
CHUNKS = ((0, 0, 64), (0, 64, 64), (1, 0, 48), (1, 48, 48), (1, 96, 32))
UNROLL = 4
SPLIT = (2, 4, 6)


def log2(size):
    assert size & (size - 1) == 0
    return size.bit_length() - 1


class Plan:
    def __init__(self, count, groups, blk_dev, head_dev):
        self.count, self.groups, self.blk, self.heads = count, groups, blk_dev, head_dev
        self.bits = log2(count)
        self.stride = groups * head_dev
        self.lanes = count * self.stride
        self.blocks = count * blk_dev
        self.req = blk_dev * R
        self.per_head = blk_dev + 2 + G
        self.own = blk_dev * head_dev
        most = max(2, (self.req + count - 1) // count)
        bound = (count // 2) * most * head_dev
        self.full = [min(self.own << s, bound) for s in range(self.bits)]
        self.base = [sum(self.full[:s]) for s in range(self.bits)]
        self.cfull = [
            min((blk_dev - 1) << s, blk_dev << (self.bits - 1 - s)) for s in range(self.bits)
        ]
        self.cbase = [sum(self.cfull[:s]) for s in range(self.bits)]
        self.width = -(-max(self.full + self.cfull) // LANES) * LANES

    def sizes(self, full, shares):
        out = []
        for s in range(self.bits):
            share = shares[0] if s == 0 else shares[2] if s == self.bits - 1 else shares[1]
            out.append(min(full[s], max(1, math.ceil(full[s] * share))))
        return out

    def route_sizes(self):
        return [self.sizes(self.full, shares) for shares in ROUTE_SHARES]

    def pack_sizes(self):
        return [self.sizes(self.cfull, shares) for shares in PACK_SHARES]

    def rows(self):
        return 2 * self.bits + 4


def iota(shape, axis):
    return lax.broadcasted_iota(jnp.int32, shape, axis)


def flag(cond):
    return jnp.where(cond, 1.0, 0.0)


def dot(a, b):
    return jnp.dot(
        a.astype(jnp.bfloat16), b.astype(jnp.bfloat16), preferred_element_type=jnp.float32
    )


def choose(tops, sizes):
    index = jnp.int32(len(sizes) - 1)
    for number in reversed(range(len(sizes) - 1)):
        fits = functools.reduce(
            jnp.logical_and, [top <= float(size) for top, size in zip(tops, sizes[number])]
        )
        index = jnp.where(fits, jnp.int32(number), index)
    return index


def lists_body(plan, scal, ids, own_ids, lists, table):
    me, group = scal[0], scal[1]
    T, L, hd = plan.blocks, plan.lanes, plan.heads
    lb, ls, lh = log2(plan.blk), log2(plan.stride), log2(hd)
    W = plan.width
    t = iota((T, L), 0)
    lane = iota((T, L), 1)
    holder = jnp.right_shift(lane, ls)
    need = jnp.zeros((T, L), jnp.int32)
    for k in range(plan.req):
        need = jnp.where(t == ids[k : k + 1, :], 1, need)
    near = (t >= holder * plan.blk - 1) & (t <= (holder + 1) * plan.blk)
    need = jnp.where(near | (t < G), 0, need)
    needb = need.astype(jnp.float32).astype(jnp.bfloat16)
    x = iota((L, L), 0)
    y = iota((L, L), 1)
    lower = flag(iota((T, T), 0) > iota((T, T), 1)).astype(jnp.bfloat16)
    upper = flag(iota((hd, hd), 0) < iota((hd, hd), 1)).astype(jnp.bfloat16)
    same = flag(jnp.right_shift(x, lh) == jnp.right_shift(y, lh)).astype(jnp.bfloat16)
    xe = iota((L, hd), 0)
    he = iota((L, hd), 1)
    th = iota((T, hd), 0)
    hh = iota((T, hd), 1)
    blk_of = jnp.right_shift(th, lb)
    pos_of = th & (plan.blk - 1)
    is_own = blk_of == me
    loc = jnp.where(is_own, jnp.left_shift(hh, lb) + pos_of, 0)
    slot_w = iota((T, W), 1)
    tops = []

    def order(mask):
        within = jnp.dot(lower, mask.astype(jnp.bfloat16), preferred_element_type=jnp.float32)
        cols = jnp.broadcast_to(jnp.sum(mask, axis=0, keepdims=True), (8, hd))
        return within + dot(cols, upper)[0:1, :]

    for s in range(plan.bits):
        b = plan.bits - 1 - s
        free = ((1 << b) - 1) << ls
        group_of = flag(((x ^ y) & ~free) == 0).astype(jnp.bfloat16)
        wanted = jnp.dot(needb, group_of, preferred_element_type=jnp.float32)
        into = ((jnp.right_shift(t, lb) ^ holder ^ (1 << b)) & ((2 << b) - 1)) == 0
        recv = flag((wanted > 0.5) & into)
        cols = jnp.broadcast_to(jnp.sum(recv, axis=0, keepdims=True), (8, L))
        tops.append(jnp.max(dot(cols, same)))
        recvb = recv.astype(jnp.bfloat16)
        mine = flag(xe == me * plan.stride + group * hd + he).astype(jnp.bfloat16)
        theirs = flag(xe == (me ^ (1 << b)) * plan.stride + group * hd + he).astype(jnp.bfloat16)
        got = jnp.dot(recvb, mine, preferred_element_type=jnp.float32)
        sent = jnp.dot(recvb, theirs, preferred_element_type=jnp.float32)
        place = jnp.where(sent > 0.5, order(sent).astype(jnp.int32), -1)
        line = jnp.zeros((1, W), jnp.int32)
        for h in range(hd):
            hit = place[:, h : h + 1] == slot_w
            line = line + jnp.sum(
                jnp.where(hit, loc[:, h : h + 1] + 1, 0), axis=0, keepdims=True
            )
        lists[s : s + 1, :] = line
        loc = jnp.where(
            got > 0.5, plan.own + plan.base[s] + order(got).astype(jnp.int32), loc
        )
    per = plan.per_head
    at = jnp.where(is_own, hh * per + 1 + pos_of, loc + hd * (per - plan.blk))
    at = jnp.where(th == me * plan.blk - 1, hh * per, at)
    at = jnp.where(th == (me + 1) * plan.blk, hh * per + 1 + plan.blk, at)
    at = jnp.where((th < G) & ~is_own, hh * per + 2 + plan.blk + th, at)
    for k in range(plan.req):
        hit = th == own_ids[k : k + 1, :]
        table[k : k + 1, 0:hd] = jnp.sum(jnp.where(hit, at, 0), axis=0, keepdims=True)

    kept = jnp.zeros((T, L), jnp.int32)
    head_lane = (jnp.right_shift(t, lb) == holder) & ((lane & (plan.stride - 1)) == 0)
    for i in range(plan.blk):
        hit = head_lane & ((t & (plan.blk - 1)) == i)
        kept = kept + jnp.where(hit, ids[plan.req + i : plan.req + i + 1, :], 0)
    kept = jnp.broadcast_to(jnp.sum(kept, axis=1, keepdims=True), (T, W))
    tw = iota((T, W), 0)
    dev = jnp.right_shift(tw, lb)

    def before(mask):
        return jnp.dot(
            lower, mask.astype(jnp.float32).astype(jnp.bfloat16), preferred_element_type=jnp.float32
        ).astype(jnp.int32)

    rank = before(kept)
    dest = jnp.right_shift(rank, lb)
    cloc = jnp.where(dev == me, tw & (plan.blk - 1), 0)
    ctops = []
    for s in range(plan.bits):
        b = plan.bits - 1 - s
        ok = (kept > 0) & (jnp.right_shift(dest ^ slot_w, b) == 0)
        ok = ok & (((dev ^ slot_w ^ (1 << b)) & ((2 << b) - 1)) == 0)
        recv = jnp.where(ok, 1, 0)
        ctops.append(jnp.max(jnp.sum(recv.astype(jnp.float32), axis=0, keepdims=True)))
        got = jnp.sum(jnp.where(slot_w == me, recv, 0), axis=1, keepdims=True)
        sent = jnp.sum(jnp.where(slot_w == (me ^ (1 << b)), recv, 0), axis=1, keepdims=True)
        got = jnp.broadcast_to(got, (T, W))
        sent = jnp.broadcast_to(sent, (T, W))
        hit = (sent > 0) & (before(sent) == slot_w)
        row = plan.bits + s
        lists[row : row + 1, :] = jnp.sum(jnp.where(hit, cloc + 1, 0), axis=0, keepdims=True)
        cloc = jnp.where(got > 0, plan.blk + plan.cbase[s] + before(got), cloc)
    row = 2 * plan.bits
    hit = (kept > 0) & (rank == me * plan.blk + slot_w) & (slot_w < plan.blk)
    lists[row : row + 1, :] = jnp.sum(jnp.where(hit, cloc + 1, 0), axis=0, keepdims=True)
    both = [a + c for a, c in zip(plan.route_sizes(), plan.pack_sizes())]
    lists[row + 1 : row + 2, :] = jnp.broadcast_to(choose(tops + ctops, both), (1, W))
    first = jnp.sum(jnp.where(tw < me * plan.blk, kept, 0), axis=0, keepdims=True)
    hit = (kept > 0) & (dev == me) & (rank - first == slot_w)
    lists[row + 2 : row + 3, :] = jnp.sum(
        jnp.where(hit, tw & (plan.blk - 1), 0), axis=0, keepdims=True
    )
    lists[row + 3 : row + 4, :] = jnp.sum(
        jnp.where((dev == me), kept, 0), axis=0, keepdims=True
    )


SMEM = pl.BlockSpec(memory_space=pltpu.SMEM)
VMEM = pl.BlockSpec(memory_space=pltpu.VMEM)
HBM = pl.BlockSpec(memory_space=pltpu.HBM)
ANY = pl.BlockSpec(memory_space=pl.ANY)


def make_lists(plan, scal, ids, own_ids):
    return pl.pallas_call(
        functools.partial(lists_body, plan),
        out_shape=(
            jax.ShapeDtypeStruct((plan.rows(), plan.width), jnp.int32),
            jax.ShapeDtypeStruct((plan.req, LANES), jnp.int32),
        ),
        in_specs=[SMEM, VMEM, VMEM],
        out_specs=(VMEM, VMEM),
        name="make_lists",
    )(scal, ids, own_ids)


def pack_body(row, size, bases, own_part, rows, lists, *refs):
    sources, out = refs[1:-1], refs[-1]

    def step(j, carry):
        code = jnp.maximum(lists[row, j] - 1, 0)
        target = pl.ds(pl.multiple_of(j * rows, rows), rows)

        @pl.when(code < bases[0])
        def _():
            out[target, :] = own_part(sources[0], code)

        for number, source in enumerate(sources[1:]):
            low = bases[number]

            @pl.when((code >= low) & (code < bases[number + 1]))
            def _():
                at = pl.multiple_of((code - low) * rows, rows)
                out[target, :] = source[pl.ds(at, rows), :]

        return carry

    lax.fori_loop(0, size, step, 0)


def pack(row, size, bases, own_part, rows, lists, after, sources, width):
    return pl.pallas_call(
        functools.partial(pack_body, row, size, bases, own_part, rows),
        out_shape=jax.ShapeDtypeStruct((size * rows, width), jnp.bfloat16),
        in_specs=[SMEM, ANY] + [VMEM] * len(sources),
        out_specs=VMEM,
    )(lists, after, *sources)


def either_body(after, scal, a, b, out):
    @pl.when(scal[2] == 0)
    def _():
        out[...] = a[...]

    @pl.when(scal[2] != 0)
    def _():
        out[...] = b[...]


def either(after, cond, a, b):
    return pl.pallas_call(
        either_body,
        out_shape=jax.ShapeDtypeStruct(a.shape, a.dtype),
        in_specs=[ANY, SMEM, VMEM, VMEM],
        out_specs=VMEM,
        name="either",
    )(after, cond, a, b)


def edges_body(after, keys, values, low, high, first_keys, first_values):
    tokens, width = keys.shape
    low[:, :width] = keys[tokens - B : tokens, :]
    low[:, width:] = values[tokens - B : tokens, :]
    high[:, :width] = keys[:B, :]
    high[:, width:] = values[:B, :]
    first_keys[...] = keys[: G * B, :]
    first_values[...] = values[: G * B, :]


def edges(after, keys, values):
    width, dtype = keys.shape[1], keys.dtype
    block = jax.ShapeDtypeStruct((B, 2 * width), dtype)
    shared = jax.ShapeDtypeStruct((G * B, width), dtype)
    return pl.pallas_call(
        edges_body,
        out_shape=(block, block, shared, shared),
        in_specs=[ANY, VMEM, VMEM],
        out_specs=(VMEM,) * 4,
        name="edges",
    )(after, keys, values)


def hold_body(after, before, x, out):
    pass


def hold(after, before, x):
    return pl.pallas_call(
        hold_body,
        out_shape=jax.ShapeDtypeStruct(x.shape, x.dtype),
        in_specs=[ANY, ANY, ANY],
        out_specs=ANY,
        input_output_aliases={2: 0},
        name="hold",
    )(after, before, x)


def tile_part(heads_bits, first, rows):
    def read(own, code):
        head = jnp.right_shift(code, heads_bits)
        pos = code & ((1 << heads_bits) - 1)
        at = pl.multiple_of(pos * B + first, 16)
        return own[pl.ds(at, rows), pl.ds(pl.multiple_of(head * DH, DH), DH)]

    return read


def block_part(own, code):
    return own[pl.ds(pl.multiple_of(code * B, B), B), :]


def final_body(row, slots, bases, widths, lists, *refs):
    out = refs[-1]
    per = (len(refs) - 1) // len(widths)

    def step(j, carry):
        code = lists[row, j]
        target = pl.ds(pl.multiple_of(j * B, B), B)

        @pl.when(code == 0)
        def _():
            out[target, :] = jnp.zeros((B, out.shape[1]), out.dtype)

        for number in range(per):
            low = 0 if number == 0 else bases[number - 1]

            @pl.when((code - 1 >= low) & (code - 1 < bases[number]))
            def _():
                at = pl.multiple_of((code - 1 - low) * B, B)
                for part, width in enumerate(widths):
                    first = sum(widths[:part])
                    out[target, first : first + width] = refs[part * per + number][
                        pl.ds(at, B), :
                    ]

        return carry

    lax.fori_loop(0, slots, step, 0)


def final(row, slots, bases, lists, sources, widths):
    return pl.pallas_call(
        functools.partial(final_body, row, slots, bases, widths),
        out_shape=jax.ShapeDtypeStruct((slots * B, sum(widths)), jnp.bfloat16),
        in_specs=[SMEM] + [VMEM] * len(sources),
        out_specs=VMEM,
        name="place_blocks",
    )(lists, *sources)


FACTOR = math.log2(math.e) / math.sqrt(DH)


def scores_of(qt, kt):
    return lax.dot_general(
        qt, kt, (((1,), (1,)), ((), ())), preferred_element_type=jnp.float32
    )


def gather_parts(scores, values, top):
    total = 0.0
    acc = 0.0
    for s, vt in zip(scores, values):
        p = jnp.exp2((s - top) * FACTOR)
        total = total + jnp.sum(p, axis=1, keepdims=True)
        acc = acc + jnp.dot(p.astype(jnp.bfloat16), vt, preferred_element_type=jnp.float32)
    return total, acc


def peak(scores):
    return functools.reduce(jnp.maximum, [jnp.max(s, axis=1, keepdims=True) for s in scores])


def start_near(plan, heads, own, low, high, shared, first, pool, sem, copies):
    wide = plan.heads * DH
    for h in heads:
        cols = pl.ds(h * DH, DH)
        there = pl.ds(first * wide + h * DH, DH)
        for source, at, tiles in (
            (low.at[:, there], 0, 1),
            (own.at[:, cols], 1, plan.blk),
            (high.at[:, there], 1 + plan.blk, 1),
            (shared.at[:, cols], 2 + plan.blk, G),
        ):
            copy = pltpu.make_async_copy(
                source,
                pool.at[pl.ds((h * plan.per_head + at) * B, tiles * B), :],
                sem.at[len(copies)],
            )
            copy.start()
            copies.append(copy)


def parts_of(which):
    return [(first, rows) for kind, first, rows in CHUNKS if kind == which]


def start_far(plan, sizes, which, chunks, pool, sem, copies):
    for part, (first, rows) in enumerate(parts_of(which)):
        for s in range(plan.bits):
            copy = pltpu.make_async_copy(
                chunks[part * plan.bits + s],
                pool.at[pl.ds(plan.base[s], sizes[s]), pl.ds(first, rows), :],
                sem.at[len(copies)],
            )
            copy.start()
            copies.append(copy)


def tile_reader(plan, near_pool, far_pool, at):
    split = plan.heads * plan.per_head
    inside = at < split
    row = pl.multiple_of(jnp.where(inside, at, 0) * B, B)
    near = near_pool[pl.ds(row, B), :]
    far = far_pool[jnp.where(inside, 0, at - split)]
    return jnp.where(inside, near, far)


def put_stats(stat, rows, hd, h, top, total):
    lane = lax.broadcasted_iota(jnp.int32, (B, LANES), 1)
    old = stat[rows, :]
    stat[rows, :] = jnp.where(lane == h, top, jnp.where(lane == hd + h, total, old))


def near_body(plan, heads, lists, scal, after, q, *refs):
    k, v, low, high, shared_k, shared_v, acc_out, stat_out, kp, vp, sem = refs
    blk, hd, per = plan.blk, plan.heads, plan.per_head
    copies = []
    start_near(plan, heads, k, low, high, shared_k, 0, kp, sem, copies)
    start_near(plan, heads, v, low, high, shared_v, 1, vp, sem, copies)
    for copy in copies:
        copy.wait()
    me = scal[0]
    row = 2 * plan.bits
    win = 3 * B

    def step(kk, carry):
        i = lists[row + 2, kk]
        first = (me * blk + i) == 0
        last = (me * blk + i) == plan.blocks - 1
        col = lax.broadcasted_iota(jnp.int32, (B, win), 1)
        dead = (first & (col < B)) | (last & (col >= 2 * B))
        rows = pl.ds(pl.multiple_of(i * B, B), B)
        for number, h in enumerate(heads):
            qt = q[rows, h * DH : (h + 1) * DH]
            spans = (
                pl.ds(pl.multiple_of((h * per + i) * B, B), win),
                pl.ds((h * per + 2 + blk) * B, G * B),
            )
            scores = [scores_of(qt, kp[span, :]) for span in spans]
            scores[0] = jnp.where(dead, neg_big, scores[0])
            top = peak(scores)
            total, acc = gather_parts(scores, [vp[span, :] for span in spans], top)
            acc_out[rows, number * DH : (number + 1) * DH] = acc
            stat_out[rows, h : h + 1] = top
            stat_out[rows, hd + h : hd + h + 1] = total
        return carry

    lax.fori_loop(0, lists[row + 3, 0], step, 0)


def near_attend(plan, heads, lists, scal, after, q, ins):
    pool = plan.heads * plan.per_head * B
    return pl.pallas_call(
        functools.partial(near_body, plan, heads),
        out_shape=(
            jax.ShapeDtypeStruct((q.shape[0], len(heads) * DH), jnp.float32),
            jax.ShapeDtypeStruct((q.shape[0], LANES), jnp.float32),
        ),
        in_specs=[SMEM, SMEM, ANY, VMEM] + [HBM] * len(ins),
        out_specs=(VMEM, VMEM),
        scratch_shapes=[
            pltpu.VMEM((pool, DH), jnp.bfloat16),
            pltpu.VMEM((pool, DH), jnp.bfloat16),
            pltpu.SemaphoreType.DMA((8 * plan.heads,)),
        ],
        name="near_attend",
    )(lists, scal, after, q, *ins)


def far_scores_body(plan, sizes, lists, table, after, q, k, low, high, shared, *refs):
    count = len(parts_of(0)) * plan.bits
    chunks, (p_out, stat_out), (near, far, sem) = refs[:count], refs[count : count + 2], refs[count + 2 :]
    hd = plan.heads
    copies = []
    start_far(plan, sizes, 0, chunks, far, sem, copies)
    start_near(plan, range(hd), k, low, high, shared, 0, near, sem, copies)
    for copy in copies:
        copy.wait()
    row = 2 * plan.bits

    def step(kk, carry):
        i = lists[row + 2, kk]
        rows = pl.ds(pl.multiple_of(i * B, B), B)

        def some_heads(g, carry):
            for n in range(UNROLL):
                h = g * UNROLL + n
                qt = q[rows, pl.ds(pl.multiple_of(h * DH, DH), DH)]
                scores = [
                    scores_of(qt, tile_reader(plan, near, far, table[i * R + r, h]))
                    for r in range(R)
                ]
                top = peak(scores)
                total = 0.0
                for r, s in enumerate(scores):
                    p = jnp.exp2((s - top) * FACTOR)
                    total = total + jnp.sum(p, axis=1, keepdims=True)
                    at = pl.multiple_of((h * R + r) * B, B)
                    p_out[rows, pl.ds(at, B)] = p.astype(jnp.bfloat16)
                put_stats(stat_out, rows, hd, h, top, total)
            return carry

        return lax.fori_loop(0, hd // UNROLL, some_heads, carry)

    lax.fori_loop(0, lists[row + 3, 0], step, 0)


def pools_of(plan):
    return [
        pltpu.VMEM((plan.heads * plan.per_head * B, DH), jnp.bfloat16),
        pltpu.VMEM((sum(plan.full), B, DH), jnp.bfloat16),
        pltpu.SemaphoreType.DMA((4 * plan.heads + len(CHUNKS) * plan.bits,)),
    ]


def far_scores(plan, sizes, lists, table, after, q, k, low, high, shared, chunks):
    return pl.pallas_call(
        functools.partial(far_scores_body, plan, sizes),
        out_shape=(
            jax.ShapeDtypeStruct((q.shape[0], plan.heads * R * B), jnp.bfloat16),
            jax.ShapeDtypeStruct((q.shape[0], LANES), jnp.float32),
        ),
        in_specs=[SMEM, SMEM, ANY, VMEM] + [HBM] * (4 + len(chunks)),
        out_specs=(VMEM, VMEM),
        scratch_shapes=pools_of(plan),
        name="far_scores",
    )(lists, table, after, q, k, low, high, shared, *chunks)


def far_values_body(plan, sizes, heads, lists, table, after, p, pstat, acc_in, stat, v, low, high,
                    shared, *refs):
    count = len(parts_of(1)) * plan.bits
    chunks, out, (near, far, sem) = refs[:count], refs[count], refs[count + 1 :]
    hd = plan.heads
    copies = []
    start_far(plan, sizes, 1, chunks, far, sem, copies)
    start_near(plan, heads, v, low, high, shared, 1, near, sem, copies)
    for copy in copies:
        copy.wait()
    row = 2 * plan.bits

    def step(kk, carry):
        i = lists[row + 2, kk]
        rows = pl.ds(pl.multiple_of(i * B, B), B)
        for number, h in enumerate(heads):
            acc = 0.0
            for r in range(R):
                acc = acc + jnp.dot(
                    p[rows, (number * R + r) * B : (number * R + r + 1) * B],
                    tile_reader(plan, near, far, table[i * R + r, h]),
                    preferred_element_type=jnp.float32,
                )
            far_top, near_top = pstat[rows, h : h + 1], stat[rows, h : h + 1]
            top = jnp.maximum(far_top, near_top)
            a = jnp.exp2((far_top - top) * FACTOR)
            c = jnp.exp2((near_top - top) * FACTOR)
            total = a * pstat[rows, hd + h : hd + h + 1] + c * stat[rows, hd + h : hd + h + 1]
            scale = 1.0 / total
            acc = (a * scale) * acc + (c * scale) * acc_in[rows, number * DH : (number + 1) * DH]
            out[rows, number * DH : (number + 1) * DH] = acc.astype(jnp.bfloat16)
        return carry

    lax.fori_loop(0, lists[row + 3, 0], step, 0)


def far_values(plan, sizes, heads, lists, table, after, p, pstat, acc, stat, v, low, high, shared,
               chunks):
    size = len(heads)
    half = acc.shape[1] // DH
    assert heads[0] % size == 0 and half % size == 0

    def of_team(x, width, first):
        return pl.BlockSpec((x.shape[0], size * width), lambda _: (0, first // size))

    return pl.pallas_call(
        functools.partial(far_values_body, plan, sizes, heads),
        out_shape=jax.ShapeDtypeStruct((p.shape[0], len(heads) * DH), jnp.bfloat16),
        grid=(1,),
        in_specs=[SMEM, SMEM, ANY, of_team(p, R * B, heads[0]), VMEM,
                  of_team(acc, DH, heads[0] % half), VMEM]
        + [HBM] * (4 + len(chunks)),
        out_specs=VMEM,
        scratch_shapes=pools_of(plan),
        name="far_values",
    )(lists, table, after, p, pstat, acc, stat, v, low, high, shared, *chunks)


def body(queries, keys, values, random_holder, random_offset, keep):
    tok_dev, width_dev = queries.shape
    blk_dev = tok_dev // B
    head_dev = width_dev // DH
    count = lax.axis_size("seq")
    groups = lax.axis_size("head")
    plan = Plan(count, groups, blk_dev, head_dev)
    bits = plan.bits
    me = lax.axis_index("seq")
    scal = jnp.stack((me, lax.axis_index("head"))).astype(jnp.int32)

    ids = (random_holder * blk_dev + random_offset).reshape(head_dev, plan.req).T
    asked = jnp.where(jnp.repeat(keep, R)[:, None] > 0, ids, -1)
    mine = jnp.concatenate((asked, jnp.broadcast_to(keep[:, None], (blk_dev, head_dev))), axis=0)
    everyone = lax.all_to_all(
        jnp.broadcast_to(mine[None], (count * groups,) + mine.shape),
        ("seq", "head"), split_axis=0, concat_axis=0, tiled=True,
    )
    everyone = jnp.transpose(everyone, (1, 0, 2)).reshape(mine.shape[0], plan.lanes)
    lists, table = make_lists(plan, scal, everyone, ids)

    blk_bits = log2(blk_dev)
    row = 2 * bits
    cuts = [0] + [cut for cut in SPLIT if cut < head_dev] + [head_dev]
    teams = [range(low, high) for low, high in zip(cuts, cuts[1:])]
    flags = lambda cond: jnp.concatenate((scal, cond.astype(jnp.int32)[None]))
    odd = flags((me & 1) == 1)

    def branch(sizes, csizes):
        def steps(queries, keys, values, lists, table, scal, odd):
            got = [[] for _ in CHUNKS]
            last = [lists]

            def run_after(fn, *args):
                out = fn(last[0], *args)
                last[0] = out[0] if isinstance(out, (tuple, list)) else out
                return out

            def hop(x, pairs):
                return lax.ppermute(x, "seq", pairs)

            def swap(x, bit, count, down_only=False):
                return hop(x, [(i, i ^ bit) for i in range(count) if not down_only or i & bit])

            def packed_tiles(s, chunk):
                which, first, rows = CHUNKS[chunk]
                bases = [plan.own + at for at in plan.base[: s + 1]]
                return run_after(
                    lambda after: pack(
                        s, sizes[s], bases, tile_part(blk_bits, first, rows), rows, lists, after,
                        [(keys, values)[which]] + got[chunk], DH,
                    )
                )

            def stage(s, chunk):
                got[chunk].append(swap(packed_tiles(s, chunk), count >> (s + 1), count))

            def tiles(which):
                return [
                    x.reshape(-1, rows, DH)
                    for (kind, first, rows), stages in zip(CHUNKS, got)
                    if kind == which
                    for x in stages
                ]

            def begin(chunk, packed):
                packed = run_after(lambda after: hold(after, got[chunk - 1][0], packed))
                got[chunk].append(swap(packed, count >> 1, count))

            stage(0, 0)
            low, high, first_keys, first_values = run_after(edges, keys, values)
            low = hop(low, [(i, i + 1) for i in range(count - 1)])
            high = hop(high, [(i + 1, i) for i in range(count - 1)])
            beside = hop(first_values, [(0, 1)])
            coming = packed_tiles(0, 1)
            held = run_after(either, odd, first_keys, beside)
            spreads = []
            for s in range(bits - 1):
                bit = count >> (s + 1)
                spreads.append(
                    (bit, [(i + j, i + j + bit) for i in range(0, count, 2 * bit) for j in (0, 1)])
                )
            chunks = len(CHUNKS)
            nears = []

            def near_half(number):
                half = head_dev // 2
                return run_after(
                    lambda after: near_attend(
                        plan, range(number * half, (number + 1) * half), lists, scal, after,
                        queries, [keys, values, low, high, shared_keys, shared_values],
                    )
                )

            for step in range(max(chunks + bits - 1, len(spreads) + 2)):
                there = None
                if step < len(spreads):
                    bit, pairs = spreads[step]
                    there = hop(held, pairs)
                elif step == len(spreads):
                    there = swap(held, 1, count)
                if step + 1 < chunks:
                    begin(step + 1, coming)
                for s in range(1, bits):
                    if 0 <= step + 1 - s < chunks:
                        stage(s, step + 1 - s)
                    if s == 1 and step + 2 < chunks:
                        coming = packed_tiles(0, step + 2)
                if step < len(spreads):
                    held = run_after(either, flags((me & bit) != 0), held, there)
                elif step == len(spreads):
                    shared_keys = run_after(either, odd, held, there)
                    shared_values = run_after(either, odd, there, held)
                if step == 1:
                    low = run_after(hold, high, low)
                if step in (len(spreads), len(spreads) + 1):
                    nears.append(near_half(step - len(spreads)))
            p, pstat = run_after(
                lambda after: far_scores(
                    plan, sizes, lists, table, after, queries, keys, low, high, shared_keys,
                    tiles(0),
                )
            )

            sources = []

            def pack_stage(s, held):
                bases = [plan.blk + at for at in plan.cbase[: s + 1]]
                packed = run_after(
                    lambda after: pack(
                        bits + s, csizes[s], bases, block_part, B, lists, after, held,
                        held[0].shape[1],
                    )
                )
                held.append(swap(packed, count >> (s + 1), count, s == 0))

            for step in range(len(teams) + 2 * (bits - 1)):
                if step < len(teams):
                    heads = teams[step]
                    acc, stat = nears[heads[0] // (head_dev // 2)]
                    attended = run_after(
                        lambda after: far_values(
                            plan, sizes, heads, lists, table, after, p, pstat, acc, stat, values,
                            low, high, shared_values, tiles(1),
                        )
                    )
                    sources.append([attended])
                    pack_stage(0, sources[step])
                for s in reversed(range(1, bits)):
                    if 0 <= step - 2 * s < len(teams):
                        pack_stage(s, sources[step - 2 * s])
            bases = [plan.blk + at for at in plan.cbase + [sum(plan.cfull)]]
            widths = [len(heads) * DH for heads in teams]
            return final(row, blk_dev, bases, lists, sum(sources, []), widths)

        return steps

    return lax.switch(
        lists[row + 1, 0],
        [branch(a, c) for a, c in zip(plan.route_sizes(), plan.pack_sizes())],
        queries, keys, values, lists, table, scal, odd,
    )


def solution(mesh):
    in_specs = (
        P("seq", "head"),
        P("seq", "head"),
        P("seq", "head"),
        P("head", "seq", None),
        P("head", "seq", None),
        P("seq"),
    )
    out_specs = P("seq", "head")
    return jax.shard_map(body, mesh=mesh, in_specs=in_specs, out_specs=out_specs, check_vma=False)
```
